16 devices in a mesh: fsdp: 16 (over z, y, x, core).
Axes of the slice: x: 2, y: 2, z: 2, core: 2. Of those that a mesh axis runs over, the one named last changes fastest.
Arguments:
- tokens: int32 [32, 512], P('fsdp')
- positions: int32 [32, 512], P('fsdp')
- embed_table: bfloat16 [49152, 960], P('fsdp')
- attn_norm: bfloat16 [960], P('fsdp')
- w_query: bfloat16 [960, 960], P('fsdp')
- w_key: bfloat16 [960, 320], P('fsdp')
- w_value: bfloat16 [960, 320], P('fsdp')
- q_norm: bfloat16 [64], replicated
- k_norm: bfloat16 [64], replicated
- w_out: bfloat16 [960, 960], P('fsdp')
- mlp_norm: bfloat16 [960], P('fsdp')
- w_gate: bfloat16 [960, 2560], P('fsdp')
- w_up: bfloat16 [960, 2560], P('fsdp')
- w_down: bfloat16 [2560, 960], P('fsdp')
- dy_out: bfloat16 [32, 512, 960], P('fsdp')
Outputs:
- output 1: bfloat16 [32, 512, 960], P('fsdp')
- output 2: float32 [49152, 960], P('fsdp')
- output 3: float32 [960], P('fsdp')
- output 4: float32 [960, 960], P('fsdp')
- output 5: float32 [960, 320], P('fsdp')
- output 6: float32 [960, 320], P('fsdp')
- output 7: float32 [64], replicated
- output 8: float32 [64], replicated
- output 9: float32 [960, 960], P('fsdp')
- output 10: float32 [960], P('fsdp')
- output 11: float32 [960, 2560], P('fsdp')
- output 12: float32 [960, 2560], P('fsdp')
- output 13: float32 [2560, 960], P('fsdp')
All inputs are finite; a program needn't handle non-finite values.
Results may differ from the reference program's by a relative error of at most 0.0185032.
Values are sent between devices in bfloat16 or wider.
A program may use at most 1 GiB of HBM per device.

```python
import math
import jax
import jax.numpy as jnp
from jax import lax

D = 960
HEADS = 15
KV_HEADS = 5
HEAD = 64
FF = 2560
VOCAB = 49152
VOCAB_P = 49152
GROUP = 16
BATCH_DEV = 2
SEQ = 512

BATCH = GROUP * BATCH_DEV
Q_PER_KV = HEADS // KV_HEADS
ROWS_SHARD = VOCAB_P // GROUP
DOC_SPAN = max(SEQ // 4, 2)
NORM_EPS = 1e-6
ROPE_THETA = 1.0e6


def draw_tokens(rng_key):
    key_list = jax.random.split(rng_key, 4)
    id_top = jax.random.randint(key_list[0], (BATCH, SEQ), 1, VOCAB + 1)
    id_mid = jax.random.randint(key_list[1], (BATCH, SEQ), 0, id_top)
    token_ids = jax.random.randint(key_list[2], (BATCH, SEQ), 0, id_mid + 1)
    shard_lo = (jnp.arange(BATCH) % GROUP) * ROWS_SHARD
    shard_hi = jnp.minimum(shard_lo + ROWS_SHARD, VOCAB)
    cover_ids = jax.random.randint(key_list[3], (BATCH,), shard_lo, shard_hi)
    token_ids = token_ids.at[:, 0].set(cover_ids)
    return token_ids.at[BATCH - 1, SEQ - 1].set(VOCAB - 1).astype(jnp.int32)


def draw_positions(rng_key):
    seq_idx = jnp.arange(SEQ, dtype=jnp.int32)[None, :]
    starts = (jax.random.randint(rng_key, (BATCH, SEQ), 0, DOC_SPAN) == 0) | (seq_idx == 0)
    last_start = lax.cummax(jnp.where(starts, seq_idx, 0), axis=1)
    return (seq_idx - last_start).astype(jnp.int32)


def setup_inputs(seed: int = 0) -> dict:
    key_list = jax.random.split(jax.random.key(seed), 16)

    def weight(key_idx, arr_shape, fan_in):
        return (jax.random.normal(key_list[key_idx], arr_shape, jnp.float32) * fan_in ** -0.5).astype(jnp.bfloat16)

    def gain_vec(key_idx, vec_len):
        return (1.0 + 0.25 * jax.random.normal(key_list[key_idx], (vec_len,), jnp.float32)).astype(jnp.bfloat16)

    table_f = jax.random.normal(key_list[2], (VOCAB_P, D), jnp.float32)
    table_f = jnp.where(jnp.arange(VOCAB_P)[:, None] < VOCAB, table_f, 0.0)
    return {
        'tokens': draw_tokens(key_list[0]),
        'positions': draw_positions(key_list[1]),
        'embed_table': table_f.astype(jnp.bfloat16),
        'attn_norm': gain_vec(3, D),
        'w_query': weight(4, (D, HEADS * HEAD), D),
        'w_key': weight(5, (D, KV_HEADS * HEAD), D),
        'w_value': weight(6, (D, KV_HEADS * HEAD), D),
        'q_norm': gain_vec(7, HEAD),
        'k_norm': gain_vec(8, HEAD),
        'w_out': weight(9, (HEADS * HEAD, D), HEADS * HEAD),
        'mlp_norm': gain_vec(10, D),
        'w_gate': weight(11, (D, FF), D),
        'w_up': weight(12, (D, FF), D),
        'w_down': weight(13, (FF, D), FF),
        'dy_out': jax.random.normal(key_list[14], (BATCH, SEQ, D), jnp.float32).astype(jnp.bfloat16),
    }


def to_bf16(values):
    return values + lax.stop_gradient(values.astype(jnp.bfloat16).astype(jnp.float32) - values)


def rms_scale(values, norm_gain):
    inv_rms = lax.rsqrt(jnp.mean(values * values, axis=-1, keepdims=True) + NORM_EPS)
    return values * inv_rms * norm_gain


def rope_tables(positions):
    half_dim = HEAD // 2
    inv_freq = jnp.exp(jnp.arange(half_dim, dtype=jnp.float32) * (-2.0 * math.log(ROPE_THETA) / HEAD))
    angles = positions.astype(jnp.float32)[:, :, None] * inv_freq
    return jnp.cos(angles), jnp.sin(angles)


def rotate(values, cos_t, sin_t):
    half_dim = values.shape[-1] // 2
    lead_half = values[..., :half_dim]
    tail_half = values[..., half_dim:]
    return jnp.concatenate([lead_half * cos_t - tail_half * sin_t, tail_half * cos_t + lead_half * sin_t], axis=-1)


def seq_attend(operands):
    q_seq, k_seq, v_seq = operands
    scores = jnp.einsum('qgrh,kgh->grqk', q_seq, k_seq) * (HEAD ** -0.5)
    causal = jnp.arange(SEQ)[:, None] >= jnp.arange(SEQ)[None, :]
    scores = jnp.where(causal, scores, -1e30)
    attn_probs = to_bf16(jax.nn.softmax(scores, axis=-1))
    return to_bf16(jnp.einsum('grqk,kgh->qgrh', attn_probs, v_seq))


def reference(tokens, positions, embed_table, attn_norm, w_query, w_key, w_value, q_norm, k_norm, w_out, mlp_norm, w_gate, w_up, w_down, dy_out):
    cos_t, sin_t = rope_tables(positions)
    cos_q = cos_t[:, :, None, None, :]
    sin_q = sin_t[:, :, None, None, :]
    cos_k = cos_t[:, :, None, :]
    sin_k = sin_t[:, :, None, :]

    def layer_fwd(x_emb, g_attn, wt_query, wt_key, wt_value, g_query, g_key, wt_out, g_mlp, wt_gate, wt_up, wt_down):
        normed = to_bf16(rms_scale(x_emb, g_attn)).reshape(BATCH * SEQ, D)
        q_proj = to_bf16(jnp.dot(normed, wt_query, preferred_element_type=jnp.float32)).reshape(BATCH, SEQ, KV_HEADS, Q_PER_KV, HEAD)
        k_proj = to_bf16(jnp.dot(normed, wt_key, preferred_element_type=jnp.float32)).reshape(BATCH, SEQ, KV_HEADS, HEAD)
        v_proj = to_bf16(jnp.dot(normed, wt_value, preferred_element_type=jnp.float32)).reshape(BATCH, SEQ, KV_HEADS, HEAD)
        q_rot = to_bf16(rotate(rms_scale(q_proj, g_query), cos_q, sin_q))
        k_rot = to_bf16(rotate(rms_scale(k_proj, g_key), cos_k, sin_k))
        attn_heads = lax.map(jax.checkpoint(seq_attend), (q_rot, k_rot, v_proj))
        attn_proj = jnp.dot(attn_heads.reshape(BATCH * SEQ, HEADS * HEAD), wt_out, preferred_element_type=jnp.float32)
        hidden = to_bf16(x_emb + attn_proj.reshape(BATCH, SEQ, D))
        mlp_in = to_bf16(rms_scale(hidden, g_mlp)).reshape(BATCH * SEQ, D)
        gate_pre = jnp.dot(mlp_in, wt_gate, preferred_element_type=jnp.float32)
        up_proj = jnp.dot(mlp_in, wt_up, preferred_element_type=jnp.float32)
        mlp_act = to_bf16(jax.nn.silu(gate_pre) * up_proj)
        mlp_proj = jnp.dot(mlp_act, wt_down, preferred_element_type=jnp.float32)
        return to_bf16(hidden + mlp_proj.reshape(BATCH, SEQ, D))

    x_emb = jnp.take(embed_table, tokens, axis=0).astype(jnp.float32)
    params = [weight_arr.astype(jnp.float32) for weight_arr in (attn_norm, w_query, w_key, w_value, q_norm, k_norm, w_out, mlp_norm, w_gate, w_up, w_down)]
    layer_out, pullback = jax.vjp(layer_fwd, x_emb, *params)
    grad_list = pullback(dy_out.astype(jnp.float32))
    d_table = jax.ops.segment_sum(grad_list[0].reshape(BATCH * SEQ, D), tokens.reshape(BATCH * SEQ), num_segments=VOCAB_P)
    return (layer_out.astype(jnp.bfloat16), d_table, grad_list[1], grad_list[2], grad_list[3], grad_list[4], grad_list[5], grad_list[6], grad_list[7], grad_list[8], grad_list[9], grad_list[10], grad_list[11])
```

```python
import math
import jax
import jax.numpy as jnp
from jax import lax
from jax.experimental import pallas as pl
from jax.experimental.pallas import tpu as pltpu
from jax.sharding import PartitionSpec as P

NORM_EPS = 1e-6
ROPE_THETA = 1.0e6
AXIS_NAME = 'fsdp'
D = 960
DP = 1024
SHARDS = 16
SUB = 60
SUBP = 64
QKVP = 1920
FF = 2560
ROWS_FF = 160
MESH_ID = pl.DeviceIdType.MESH
BITS = {'z': 8, 'y': 4, 'x': 2, 'c': 1}
AG_PIECES = ((0, 0, 896, 'xyz'), (0, 896, 1024, 'yzx'), (1, 0, DP, 'zxy'), (2, 0, FF, 'xyz'), (3, 0, FF, 'yzx'), (4, 0, DP, 'zxy'))
RS_PIECES = AG_PIECES[3:] + AG_PIECES[:3] + ((5, 0, 128, 'yzx'),)
ROW_PIECES = tuple((0, half + lo, count, order) for half in (0, 512) for lo, count, order in ((0, 176, 'xyz'), (176, 176, 'yzx'), (352, 160, 'zxy')))
ROWS = (SUBP, SUBP, SUBP, SUBP, ROWS_FF, SUBP)
COLS = (QKVP, DP, FF, FF, DP, 128)
TOKS = 1024
ROWS_TABLE = 3072
UNROLL = 8
HEADS, KV_HEADS, GROUP, HEAD, SEQ, HALF = 15, 5, 3, 64, 512, 256
GROUP_IN = 384
GROUP_OUT = 256
MIB = 1024 * 1024
FIRST_ORDER = (3, 7, 5, 1, 2, 6, 4, 0)
ANY_SPEC = pl.BlockSpec(memory_space=pl.ANY)
VMEM_SPEC = pl.BlockSpec(memory_space=pltpu.VMEM)
HOPS = ((0, 0), (0, 2), (0, 4), (0, 6), (1, 0), (1, 4), (2, 0))


def own_bits():
    me = lax.axis_index(AXIS_NAME)
    return {'z': me // 8, 'y': (me // 4) % 2, 'x': (me // 2) % 2, 'c': me % 2}


def device_at(bits, flips):
    total = 0
    for name, weight in BITS.items():
        total = total + ((1 - bits[name]) if name in flips else bits[name]) * weight
    return total


def flips_of(code, order):
    return ''.join(order[i] for i in range(3) if (code >> i) & 1)


def greet(bits):
    barrier = pltpu.get_barrier_semaphore()
    for name in BITS:
        pl.semaphore_signal(barrier, inc=1, device_id=(device_at(bits, name),), device_id_type=MESH_ID)
    pl.semaphore_wait(barrier, 4)


class Doubling:
    def __init__(self, bits, pieces, ins, outs, view, send_sem, recv_sem):
        self.bits, self.pieces, self.ins, self.outs, self.view = bits, pieces, ins, outs, view
        self.send_sem, self.recv_sem = send_sem, recv_sem
        self.started = []

    def begin(self, p, code, step, src_code):
        piece = self.pieces[p]
        a, order = piece[0], piece[3]
        shard = device_at(self.bits, flips_of(src_code, order))
        src = self.ins[a] if src_code == 0 else self.outs[a].at[shard]
        target = device_at(self.bits, 'c' if step == 3 else order[step])
        slot = 8 + src_code if step == 3 else code
        desc = pltpu.make_async_remote_copy(
            src_ref=self.view(src, piece), dst_ref=self.view(self.outs[a].at[shard], piece),
            send_sem=self.send_sem.at[p, slot], recv_sem=self.recv_sem.at[p, slot],
            device_id=(target,), device_id_type=MESH_ID)
        desc.start()
        self.started.append(desc)

    def arrived(self, p, slot):
        piece = self.pieces[p]
        flips = flips_of(slot % 8, piece[3]) + ('c' if slot >= 8 else '')
        dst = self.view(self.outs[piece[0]].at[device_at(self.bits, flips)], piece)
        pltpu.make_async_remote_copy(
            src_ref=dst, dst_ref=dst, send_sem=self.send_sem.at[p, slot], recv_sem=self.recv_sem.at[p, slot],
            device_id=(device_at(self.bits, 'c'),), device_id_type=MESH_ID).wait_recv()

    def open(self):
        for step in range(3):
            for p in range(len(self.pieces)):
                self.begin(p, 1 << step, step, 0)
        for p in range(len(self.pieces)):
            self.begin(p, 0, 3, 0)

    def forward(self, code):
        top = 0 if code == 1 else (1 if code < 4 else 2)
        for p in range(len(self.pieces)):
            self.arrived(p, code)
            for step in range(top + 1, 3):
                self.begin(p, code | (1 << step), step, code)
            self.begin(p, 0, 3, code)

    def close(self):
        for code in range(8):
            for p in range(len(self.pieces)):
                self.arrived(p, 8 + code)
        for desc in self.started:
            desc.wait_send()


def columns_of(ref, piece):
    return ref.at[:, pl.ds(piece[1], piece[2])]


def rows_of(ref, piece):
    return ref.at[pl.ds(piece[1], piece[2])]


class Halving:
    def __init__(self, bits, pieces, source, acc, got, send_sem, recv_sem):
        self.bits, self.pieces, self.source, self.acc, self.got = bits, pieces, source, acc, got
        self.send_sem, self.recv_sem = send_sem, recv_sem

    def cross(self, p, code):
        return pltpu.make_async_remote_copy(
            src_ref=self.source(p, code), dst_ref=self.acc[p].at[code],
            send_sem=self.send_sem.at[p, code], recv_sem=self.recv_sem.at[p, code],
            device_id=(device_at(self.bits, 'c'),), device_id_type=MESH_ID)

    def hop(self, p, step, code):
        sem = UNROLL + HOPS.index((step, code))
        return pltpu.make_async_remote_copy(
            src_ref=self.acc[p].at[code | (1 << step)], dst_ref=self.got[step][p].at[code >> (step + 1)],
            send_sem=self.send_sem.at[p, sem], recv_sem=self.recv_sem.at[p, sem],
            device_id=(device_at(self.bits, self.pieces[p][3][step]),), device_id_type=MESH_ID)

    def total(self, p, code, at, steps):
        total = self.acc[p][code, at]
        for step in steps:
            total = total + self.got[step][p][code >> (step + 1), at]
        return total

    def add(self, p, code, steps, put=None):
        for step in steps:
            self.hop(p, step, code).wait_recv()

        def chunk(i, carry):
            at = pl.ds(pl.multiple_of(i * UNROLL, UNROLL), UNROLL)
            total = self.total(p, code, at, steps)
            if put is None:
                self.acc[p][code, at] = total
            else:
                put(p, at, total)
            return carry

        lax.fori_loop(0, self.acc[p].shape[1] // UNROLL, chunk, 0)

    def first(self, fill):
        for n, code in enumerate(FIRST_ORDER):
            for p in range(len(self.pieces)):
                self.cross(p, code).wait_recv()
                fill(p, n, code)
                if code & 1:
                    self.hop(p, 0, code - 1).start()

    def rest(self, put):
        pieces = range(len(self.pieces))
        for code in (2, 6):
            for p in pieces:
                self.add(p, code, (0,))
                self.hop(p, 1, code - 2).start()
        for p in pieces:
            self.add(p, 4, (0, 1))
            self.hop(p, 2, 0).start()
        for p in pieces:
            self.add(p, 0, (0, 1, 2), put)
        for p in pieces:
            for code in FIRST_ORDER:
                self.cross(p, code).wait_send()
            for step, code in HOPS:
                self.hop(p, step, code).wait_send()


def columns_of(ref, piece):
    return ref.at[:, pl.ds(piece[1], piece[2])]


def rows_of(ref, piece):
    return ref.at[pl.ds(piece[1], piece[2])]


def sems(count):
    return [pltpu.SemaphoreType.DMA((count, 16))] * 2


def cost(gflops):
    return pl.CostEstimate(flops=gflops * 10 ** 9, bytes_accessed=10 ** 8, transcendentals=0)


def front_body(*refs):
    num = 5
    np_ = len(ROW_PIECES)
    where_ref, table_ref, *refs = refs
    ins, outs, x_ref, stage, rest = refs[:num], refs[num:2 * num], refs[2 * num], refs[2 * num + 1:3 * num + 1], refs[3 * num + 1:]
    away, acc, *got = (rest[i * np_:(i + 1) * np_] for i in range(num))
    w_send, w_recv, load_sem, store_sem, x_send, x_recv = rest[num * np_:]
    bits = own_bits()
    pieces = range(np_)
    loads = [pltpu.make_async_copy(ins[a], stage[a], load_sem.at[a]) for a in range(num)]
    stores = [pltpu.make_async_copy(stage[a], outs[a].at[device_at(bits, '')], store_sem.at[a]) for a in range(num)]
    for load in loads:
        load.start()
    greet(bits)
    ring = Doubling(bits, AG_PIECES, ins, outs, columns_of, w_send, w_recv)
    ring.open()
    tree = Halving(bits, ROW_PIECES, lambda p, code: away[p].at[code], acc, got, x_send, x_recv)

    def pick(p, code, other):
        first, count, order = ROW_PIECES[p][1:]
        base = device_at(bits, flips_of(code, order) + ('c' if other else '')) * TOKS + first

        def step(i, carry):
            for k in range(UNROLL):
                t = i * UNROLL + k
                row = table_ref[where_ref[base + t]]
                if other:
                    away[p][code, t] = row
                else:
                    acc[p][code, t] = acc[p][code, t] + row
            return carry

        lax.fori_loop(0, count // UNROLL, step, 0)

    for code in FIRST_ORDER:
        for p in pieces:
            pick(p, code, True)
            tree.cross(p, code).start()
    for load, store in zip(loads, stores):
        load.wait()
        store.start()
    for code in range(1, 4):
        ring.forward(code)
    tree.first(lambda p, n, code: pick(p, code, False))
    for code in range(4, UNROLL):
        ring.forward(code)

    def put(p, at, total):
        x_ref[pl.ds(ROW_PIECES[p][1] + at.start, UNROLL)] = total

    tree.rest(put)
    ring.close()
    for store in stores:
        store.wait()


def front(where, table, shards):
    num = len(shards)
    scratch = [pltpu.VMEM((ROWS[a], COLS[a]), jnp.bfloat16) for a in range(num)]
    for lead in (8, 8, 4, 2, 1):
        scratch += [pltpu.VMEM((lead, piece[2], 8, 128), jnp.bfloat16) for piece in ROW_PIECES]
    scratch += sems(len(AG_PIECES)) + [pltpu.SemaphoreType.DMA((num,))] * 2 + sems(len(ROW_PIECES))
    return pl.pallas_call(
        front_body,
        out_shape=tuple(jax.ShapeDtypeStruct((SHARDS, ROWS[a], COLS[a]), jnp.bfloat16) for a in range(num)) + (jax.ShapeDtypeStruct((TOKS, 8, 128), jnp.bfloat16),),
        in_specs=[pl.BlockSpec(memory_space=pltpu.SMEM), VMEM_SPEC] + [ANY_SPEC] * num,
        out_specs=(ANY_SPEC,) * num + (VMEM_SPEC,),
        scratch_shapes=scratch,
        compiler_params=pltpu.CompilerParams(collective_id=1, has_side_effects=True, vmem_limit_bytes=63 * MIB),
        cost_estimate=cost(60),
        name='front',
    )(where, table, *shards)


def rows_body(in_ref, out_ref, stage, send_sem, recv_sem, own_sem):
    bits = own_bits()
    load = pltpu.make_async_copy(in_ref, stage, own_sem.at[0])
    load.start()
    greet(bits)
    ring = Doubling(bits, ROW_PIECES, (in_ref,), (out_ref,), rows_of, send_sem, recv_sem)
    ring.open()
    load.wait()
    store = pltpu.make_async_copy(stage, out_ref.at[device_at(bits, '')], own_sem.at[1])
    store.start()
    for code in range(1, UNROLL):
        ring.forward(code)
    ring.close()
    store.wait()


def gather_rows(rows):
    return pl.pallas_call(
        rows_body,
        out_shape=jax.ShapeDtypeStruct((SHARDS, TOKS, 8, 128), jnp.float32),
        in_specs=[ANY_SPEC],
        out_specs=ANY_SPEC,
        scratch_shapes=[pltpu.VMEM((TOKS, 8, 128), jnp.float32)] + sems(len(ROW_PIECES)) + [pltpu.SemaphoreType.DMA((2,))],
        compiler_params=pltpu.CompilerParams(collective_id=3, has_side_effects=True),
        cost_estimate=cost(80),
        name='gather_rows',
    )(rows)


def scatter_body(*refs):
    num = len(ROWS)
    np_ = len(RS_PIECES)
    ins, outs, rest = refs[:num], refs[num:2 * num], refs[2 * num:]
    acc, own, *got = (rest[i * np_:(i + 1) * np_] for i in range(5))
    send_sem, recv_sem, own_sem = rest[5 * np_:]
    bits = own_bits()
    pieces = range(np_)

    def part(p, code, flips):
        shard = device_at(bits, flips_of(code, RS_PIECES[p][3]) + flips)
        return columns_of(ins[RS_PIECES[p][0]].at[shard], RS_PIECES[p])

    tree = Halving(bits, RS_PIECES, lambda p, code: part(p, code, 'c'), acc, got, send_sem, recv_sem)

    def own_copy(p, n):
        return pltpu.make_async_copy(part(p, FIRST_ORDER[n], ''), own[p].at[n % 2], own_sem.at[p, n % 2])

    for p in pieces:
        own_copy(p, 0).start()
        own_copy(p, 1).start()
    greet(bits)
    for code in FIRST_ORDER:
        for p in pieces:
            tree.cross(p, code).start()

    def fill(p, n, code):
        own_copy(p, n).wait()

        def chunk(i, carry):
            at = pl.ds(pl.multiple_of(i * UNROLL, UNROLL), UNROLL)
            acc[p][code, at] = acc[p][code, at] + own[p][n % 2, at]
            return carry

        lax.fori_loop(0, acc[p].shape[1] // UNROLL, chunk, 0)
        if n + 2 < len(FIRST_ORDER):
            own_copy(p, n + 2).start()

    def put(p, at, total):
        a, first, cols, order = RS_PIECES[p]
        outs[a][at, pl.ds(first, cols)] = total

    tree.first(fill)
    tree.rest(put)


def scatter_grads(parts):
    num = len(ROWS)
    np_ = len(RS_PIECES)
    scratch = []
    for lead in (8, 2, 4, 2, 1):
        scratch += [pltpu.VMEM((lead, ROWS[piece[0]], piece[2]), jnp.float32) for piece in RS_PIECES]
    scratch += sems(np_) + [pltpu.SemaphoreType.DMA((np_, 2))]
    return pl.pallas_call(
        scatter_body,
        out_shape=tuple(jax.ShapeDtypeStruct(shape, jnp.float32) for shape in zip(ROWS, COLS)),
        in_specs=[ANY_SPEC] * num,
        out_specs=(VMEM_SPEC,) * num,
        scratch_shapes=scratch,
        compiler_params=pltpu.CompilerParams(collective_id=2, has_side_effects=True, vmem_limit_bytes=60 * MIB),
        cost_estimate=cost(60),
        name='scatter_grads',
    )(*parts)


def spread_matrix():
    src = lax.broadcasted_iota(jnp.int32, (D, DP), 0)
    dst = lax.broadcasted_iota(jnp.int32, (D, DP), 1)
    return ((src // SUB) * SUBP + src % SUB == dst).astype(jnp.bfloat16)


def heads_matrix():
    src = lax.broadcasted_iota(jnp.int32, (KV_HEADS * GROUP_OUT, DP), 0)
    dst = lax.broadcasted_iota(jnp.int32, (KV_HEADS * GROUP_OUT, DP), 1)
    lane = src % GROUP_OUT
    feature = (src // GROUP_OUT) * GROUP * HEAD + lane
    return ((lane < GROUP * HEAD) & ((feature // SUB) * SUBP + feature % SUB == dst)).astype(jnp.bfloat16)


def matmul(spec, lhs, rhs):
    return jnp.einsum(spec, lhs, rhs, preferred_element_type=jnp.float32)


def spread(values, matrix):
    return matmul('...d,de->...e', values, matrix).astype(jnp.bfloat16)


def gather_back(values, matrix):
    return matmul('...e,de->...d', values, matrix).astype(jnp.bfloat16)


def unspread_columns(values):
    rows = values.shape[0]
    return values.reshape(rows, SHARDS, SUBP)[:, :, :SUB].reshape(rows, D)


def merge_groups(w_query, w_key, w_value, gains):
    parts = []
    for g in range(KV_HEADS):
        at = slice(g * HEAD, (g + 1) * HEAD)
        spare = jnp.pad(gains if g == 0 else gains[:, :0], ((0, 0), (0, HEAD - (2 if g == 0 else 0))))
        parts += [w_query[:, g * GROUP * HEAD:(g + 1) * GROUP * HEAD], w_key[:, at], w_value[:, at], spare]
    return jnp.concatenate(parts, axis=1)


def split_groups(merged):
    grouped = merged.reshape(merged.shape[0], KV_HEADS, GROUP_IN)
    edges = (0, GROUP * HEAD, (GROUP + 1) * HEAD, (GROUP + 2) * HEAD)
    return tuple(grouped[:, :, lo:hi].reshape(merged.shape[0], -1) for lo, hi in zip(edges, edges[1:]))


def sort_by_owner(tok):
    owner = tok // ROWS_TABLE
    onehot = (owner[:, None] == jnp.arange(SHARDS, dtype=jnp.int32)[None, :]).astype(jnp.bfloat16)
    row = lax.broadcasted_iota(jnp.int32, (TOKS, TOKS), 0)
    col = lax.broadcasted_iota(jnp.int32, (TOKS, TOKS), 1)
    rank = jnp.dot((row > col).astype(jnp.bfloat16), onehot, preferred_element_type=jnp.float32)
    count = jnp.sum(onehot.astype(jnp.float32), axis=0)
    before = lax.broadcasted_iota(jnp.int32, (SHARDS, SHARDS), 0) < lax.broadcasted_iota(jnp.int32, (SHARDS, SHARDS), 1)
    first = jnp.sum(jnp.where(before, count[:, None], 0.0), axis=0)
    place = jnp.sum(onehot.astype(jnp.float32) * (rank + first[None, :]), axis=1).astype(jnp.int32)
    order_m = (row == place[None, :]).astype(jnp.bfloat16)
    local = tok - owner * ROWS_TABLE
    halves = jnp.stack([local // 64, local % 64], axis=-1).astype(jnp.bfloat16)
    halves = jnp.dot(order_m, halves, preferred_element_type=jnp.float32).astype(jnp.int32)
    return place, halves[:, 0] * 64 + halves[:, 1], count.astype(jnp.int32), first.astype(jnp.int32)


def order_body(place_ref, in_ref, out_ref):
    def step(i, carry):
        for k in range(UNROLL):
            t = i * UNROLL + k
            out_ref[place_ref[t]] = in_ref[t]
        return carry

    lax.fori_loop(0, TOKS // UNROLL, step, 0)


def order_rows(place, rows):
    whole = pl.BlockSpec((TOKS, 8, 128), lambda i, *_: (0, 0, 0))
    return pl.pallas_call(
        order_body,
        grid_spec=pltpu.PrefetchScalarGridSpec(num_scalar_prefetch=1, grid=(1,), in_specs=[whole], out_specs=whole),
        out_shape=jax.ShapeDtypeStruct((TOKS, 8, 128), jnp.float32),
        compiler_params=pltpu.CompilerParams(vmem_limit_bytes=40 * MIB),
        name='order_rows',
    )(place, rows)


def add_body(ids_ref, first_ref, count_ref, in_ref, out_ref, acc0, acc1):
    j = pl.program_id(0)
    first = first_ref[j]
    count = count_ref[j]
    zero = jnp.zeros((UNROLL, 8, 128), jnp.float32)

    @pl.when(j == 0)
    def _():
        def clear(i, carry):
            at = pl.ds(i * UNROLL, UNROLL)
            acc0[at] = zero
            acc1[at] = zero
            return carry

        lax.fori_loop(0, ROWS_TABLE // UNROLL, clear, 0)

    def step(i, carry):
        for k in range(4):
            at = first + i * 8 + 2 * k
            r0 = ids_ref[j * TOKS + at]
            r1 = ids_ref[j * TOKS + at + 1]
            acc0[r0] = acc0[r0] + in_ref[at]
            acc1[r1] = acc1[r1] + in_ref[at + 1]
        return carry

    lax.fori_loop(0, count // 8, step, 0)

    def tail(i, carry):
        r = ids_ref[j * TOKS + first + i]
        acc0[r] = acc0[r] + in_ref[first + i]
        return carry

    lax.fori_loop((count // 8) * 8, count, tail, 0)

    @pl.when(j == SHARDS - 1)
    def _():
        def flush(i, carry):
            for part in range(UNROLL):
                at = pl.ds(pl.multiple_of((i * UNROLL + part) * 8, 8), 8)
                for k in range(8):
                    both = acc0[at, k, :] + acc1[at, k, :]
                    for half in range(2):
                        out_ref[at, pl.ds((2 * k + half) * SUB, SUB)] = both[:, half * SUBP:half * SUBP + SUB]
            return carry

        lax.fori_loop(0, ROWS_TABLE // 8 // UNROLL, flush, 0)


def add_rows(ids, first, count, rows):
    return pl.pallas_call(
        add_body,
        grid_spec=pltpu.PrefetchScalarGridSpec(
            num_scalar_prefetch=3, grid=(SHARDS,),
            in_specs=[pl.BlockSpec((TOKS, 8, 128), lambda j, *_: (j, 0, 0))],
            out_specs=pl.BlockSpec((ROWS_TABLE, D), lambda j, *_: (0, 0)),
            scratch_shapes=[pltpu.VMEM((ROWS_TABLE, 8, 128), jnp.float32)] * 2),
        out_shape=jax.ShapeDtypeStruct((ROWS_TABLE, D), jnp.float32),
        compiler_params=pltpu.CompilerParams(vmem_limit_bytes=60 * MIB),
        name='add_rows',
    )(ids, first, count, rows)


def rope_tables(positions):
    half_dim = HEAD // 2
    inv_freq = jnp.exp(jnp.arange(half_dim, dtype=jnp.float32) * (-2.0 * math.log(ROPE_THETA) / HEAD))
    angles = positions.astype(jnp.float32)[:, :, None] * inv_freq
    cos_t, sin_t = jnp.cos(angles), jnp.sin(angles)
    return jnp.concatenate([cos_t, cos_t], axis=-1), jnp.concatenate([-sin_t, sin_t], axis=-1)


def swap_halves(values):
    half_dim = HEAD // 2
    return jnp.concatenate([values[:, half_dim:], values[:, :half_dim]], axis=-1)


def norm_fwd(values, width=HEAD):
    values_f = values.astype(jnp.float32)
    inv_rms = lax.rsqrt(jnp.sum(values_f * values_f, axis=-1, keepdims=True) * (1.0 / width) + NORM_EPS)
    return values_f * inv_rms, inv_rms


def norm_bwd(grad_out, normed, inv_rms, norm_gain, width=HEAD):
    grad_normed = grad_out * norm_gain.astype(jnp.float32)
    mean_term = jnp.sum(grad_normed * normed, axis=-1, keepdims=True) * (1.0 / width)
    return inv_rms * (grad_normed - normed * mean_term)


def rope_fwd(normed, gain, cos_w, sin_w):
    scaled = normed * gain
    return (scaled * cos_w + swap_halves(scaled) * sin_w).astype(jnp.bfloat16)


def dot_nt(lhs, rhs):
    return lax.dot_general(lhs, rhs, (((1,), (1,)), ((), ())), preferred_element_type=jnp.float32)


def dot_nn(lhs, rhs):
    return lax.dot_general(lhs, rhs, (((1,), (0,)), ((), ())), preferred_element_type=jnp.float32)


def dot_tn(lhs, rhs):
    return lax.dot_general(lhs, rhs, (((0,), (0,)), ((), ())), preferred_element_type=jnp.float32)


def mask_last(scores, axis):
    split = scores.shape[axis] - HALF
    key = lax.broadcasted_iota(jnp.int32, (HALF, HALF), axis)
    query = lax.broadcasted_iota(jnp.int32, (HALF, HALF), 1 - axis)
    last = jnp.where(key <= query, lax.slice_in_dim(scores, split, split + HALF, axis=axis), -1e30)
    if split == 0:
        return last
    return jnp.concatenate([lax.slice_in_dim(scores, 0, split, axis=axis), last], axis=axis)


def softmax_of(scores, axis):
    scores = mask_last(scores * (HEAD ** -0.5), axis)
    weights = jnp.exp(scores - jnp.max(scores, axis=axis, keepdims=True))
    return weights * (1.0 / jnp.sum(weights, axis=axis, keepdims=True))


def head_of(ref, h):
    return ref[0, :, h * HEAD:(h + 1) * HEAD]


def attn_fwd_body(qkv_ref, cos_ref, sin_ref, gq_ref, gk_ref, o_ref):
    cos_w, sin_w = cos_ref[0], sin_ref[0]
    k_rot = rope_fwd(norm_fwd(head_of(qkv_ref, GROUP))[0], gk_ref[...], cos_w, sin_w)
    v_raw = head_of(qkv_ref, GROUP + 1)
    for r in range(GROUP):
        at = slice(r * HEAD, (r + 1) * HEAD)
        q_rot = rope_fwd(norm_fwd(head_of(qkv_ref, r))[0], gq_ref[...], cos_w, sin_w)
        for lo in range(0, SEQ, HALF):
            hi = lo + HALF
            probs = softmax_of(dot_nt(k_rot[:hi], q_rot[lo:hi]), 0)
            o_ref[0, lo:hi, at] = dot_tn(probs.astype(jnp.bfloat16), v_raw[:hi]).astype(jnp.bfloat16)
    o_ref[0, :, GROUP * HEAD:] = jnp.zeros((SEQ, HEAD), jnp.bfloat16)


def attn_bwd_body(qkv_ref, cos_ref, sin_ref, gq_ref, gk_ref, do_ref, d_ref, dgq_ref, dgk_ref, dq_acc, dk_acc, dv_acc):
    cos_w, sin_w = cos_ref[0], sin_ref[0]
    gain_q, gain_k = gq_ref[...], gk_ref[...]
    k_normed, k_inv = norm_fwd(head_of(qkv_ref, GROUP))
    k_rot = rope_fwd(k_normed, gain_k, cos_w, sin_w)
    v_raw = head_of(qkv_ref, GROUP + 1)
    dk_acc[...] = jnp.zeros_like(dk_acc)
    dv_acc[...] = jnp.zeros_like(dv_acc)
    gain_total = jnp.zeros((1, HEAD), jnp.float32)
    for r in range(GROUP):
        q_normed, q_inv = norm_fwd(head_of(qkv_ref, r))
        q_rot = rope_fwd(q_normed, gain_q, cos_w, sin_w)
        head_grad = head_of(do_ref, r)
        for lo in range(0, SEQ, HALF):
            hi = lo + HALF
            out_grad = head_grad[lo:hi]
            q_part = q_rot[lo:hi]
            probs = softmax_of(dot_nt(k_rot[:hi], q_part), 0)
            grad_probs = dot_nt(v_raw[:hi], out_grad)
            dv_acc[:hi] += dot_nn(probs.astype(jnp.bfloat16), out_grad)
            delta = jnp.sum(grad_probs * probs, axis=0, keepdims=True)
            grad_scores = (probs * (grad_probs - delta) * (HEAD ** -0.5)).astype(jnp.bfloat16)
            dk_acc[:hi] += dot_nn(grad_scores, q_part)
            dq_acc[lo:hi] = dot_tn(grad_scores, k_rot[:hi])
        grad_q = dq_acc[...]
        grad_q = grad_q * cos_w - swap_halves(grad_q) * sin_w
        gain_total = gain_total + jnp.sum(grad_q * q_normed, axis=0, keepdims=True)
        d_ref[0, :, r * HEAD:(r + 1) * HEAD] = norm_bwd(grad_q, q_normed, q_inv, gain_q).astype(jnp.bfloat16)
    grad_k = dk_acc[...]
    grad_k = grad_k * cos_w - swap_halves(grad_k) * sin_w
    dgq_ref[0, 0] = gain_total
    dgk_ref[0, 0] = jnp.sum(grad_k * k_normed, axis=0, keepdims=True)
    d_ref[0, :, GROUP * HEAD:(GROUP + 1) * HEAD] = norm_bwd(grad_k, k_normed, k_inv, gain_k).astype(jnp.bfloat16)
    d_ref[0, :, (GROUP + 1) * HEAD:] = jnp.concatenate([dv_acc[...], jnp.zeros((SEQ, HEAD), jnp.float32)], axis=-1).astype(jnp.bfloat16)


def attn_specs():
    def lanes(width):
        return pl.BlockSpec((1, SEQ, width), lambda b, g: (b, 0, g))

    table = pl.BlockSpec((1, SEQ, HEAD), lambda b, g: (b, 0, 0))
    gain = pl.BlockSpec((1, HEAD), lambda b, g: (0, 0))
    return lanes, [lanes(GROUP_IN), table, table, gain, gain]


def attn_fwd(qkv, *tables):
    batch_len = qkv.shape[0]
    lanes, specs = attn_specs()
    return pl.pallas_call(
        attn_fwd_body,
        grid=(batch_len, KV_HEADS),
        out_shape=jax.ShapeDtypeStruct((batch_len, SEQ, KV_HEADS * GROUP_OUT), jnp.bfloat16),
        in_specs=specs,
        out_specs=lanes(GROUP_OUT),
        compiler_params=pltpu.CompilerParams(vmem_limit_bytes=40 * MIB),
        cost_estimate=cost(8),
        name='attn_fwd',
    )(qkv, *tables)


def attn_bwd(qkv, *tables):
    batch_len = qkv.shape[0]
    lanes, specs = attn_specs()
    gain_out = pl.BlockSpec((1, 1, 1, HEAD), lambda b, g: (b, g, 0, 0))
    gain_shape = jax.ShapeDtypeStruct((batch_len, KV_HEADS, 1, HEAD), jnp.float32)
    return pl.pallas_call(
        attn_bwd_body,
        grid=(batch_len, KV_HEADS),
        out_shape=(jax.ShapeDtypeStruct(qkv.shape, jnp.bfloat16), gain_shape, gain_shape),
        in_specs=specs + [lanes(GROUP_OUT)],
        out_specs=(lanes(GROUP_IN), gain_out, gain_out),
        scratch_shapes=[pltpu.VMEM((SEQ, HEAD), jnp.float32)] * 3,
        compiler_params=pltpu.CompilerParams(vmem_limit_bytes=40 * MIB),
        cost_estimate=cost(16),
        name='attn_bwd',
    )(qkv, *tables)


def layer_fwd(x_emb, positions, weights):
    attn_norm, w_qkv, q_norm, k_norm, w_out, mlp_norm, w_gate, w_up, w_down = weights
    cos_w, sin_w = rope_tables(positions)
    gain_q = q_norm.astype(jnp.float32)[None, :]
    gain_k = k_norm.astype(jnp.float32)[None, :]
    normed1, norm1_inv = norm_fwd(x_emb, D)
    attn_in = (normed1 * attn_norm.astype(jnp.float32)).astype(jnp.bfloat16)
    attn_args = (matmul('bsd,dn->bsn', attn_in, w_qkv).astype(jnp.bfloat16), cos_w, sin_w, gain_q, gain_k)
    attn_flat = spread(attn_fwd(*attn_args), heads_matrix())
    hidden = (x_emb.astype(jnp.float32) + matmul('bsn,nd->bsd', attn_flat, w_out)).astype(jnp.bfloat16)
    normed2, norm2_inv = norm_fwd(hidden, D)
    mlp_in = (normed2 * mlp_norm.astype(jnp.float32)).astype(jnp.bfloat16)
    gate_pre = matmul('bsd,df->bsf', mlp_in, w_gate)
    up_proj = matmul('bsd,df->bsf', mlp_in, w_up)
    mlp_act = (jax.nn.silu(gate_pre) * up_proj).astype(jnp.bfloat16)
    layer_out = (hidden.astype(jnp.float32) + matmul('bsf,fd->bsd', mlp_act, w_down)).astype(jnp.bfloat16)
    return layer_out, (normed1, norm1_inv, attn_in, attn_args, attn_flat, normed2, norm2_inv, mlp_in, gate_pre, up_proj, mlp_act)


def layer_bwd(dy_out, saved_acts, weights):
    attn_norm, w_qkv, q_norm, k_norm, w_out, mlp_norm, w_gate, w_up, w_down = weights
    normed1, norm1_inv, attn_in, attn_args, attn_flat, normed2, norm2_inv, mlp_in, gate_pre, up_proj, mlp_act = saved_acts
    grad_w_down = matmul('bsf,bsd->fd', mlp_act, dy_out)
    grad_act = matmul('bsd,fd->bsf', dy_out, w_down)
    gate_sig = jax.nn.sigmoid(gate_pre)
    grad_gate = (grad_act * up_proj * gate_sig * (1.0 + gate_pre * (1.0 - gate_sig))).astype(jnp.bfloat16)
    grad_up = (grad_act * gate_pre * gate_sig).astype(jnp.bfloat16)
    grad_w_gate = matmul('bsd,bsf->df', mlp_in, grad_gate)
    grad_w_up = matmul('bsd,bsf->df', mlp_in, grad_up)
    grad_mlp_in = matmul('bsf,df->bsd', grad_gate, w_gate) + matmul('bsf,df->bsd', grad_up, w_up)
    grad_mlp_norm = jnp.sum(grad_mlp_in * normed2, axis=(0, 1))
    grad_hidden = dy_out.astype(jnp.float32) + norm_bwd(grad_mlp_in, normed2, norm2_inv, mlp_norm, D)
    hidden_b = grad_hidden.astype(jnp.bfloat16)
    grad_w_out = matmul('bsn,bsd->nd', attn_flat, hidden_b)
    grad_heads = gather_back(matmul('bsd,nd->bsn', hidden_b, w_out).astype(jnp.bfloat16), heads_matrix())
    grad_qkv, gains_q, gains_k = attn_bwd(*attn_args, grad_heads)
    grad_w_qkv = matmul('bsd,bsn->dn', attn_in, grad_qkv)
    grad_attn_in = matmul('bsn,dn->bsd', grad_qkv, w_qkv)
    grad_attn_norm = jnp.sum(grad_attn_in * normed1, axis=(0, 1))
    grad_x_emb = grad_hidden + norm_bwd(grad_attn_in, normed1, norm1_inv, attn_norm, D)
    head_grads = [jnp.tile(jnp.sum(gains, axis=(0, 1, 2)), SHARDS) for gains in (gains_q, gains_k)]
    small = jnp.stack([grad_attn_norm, grad_mlp_norm] + head_grads, axis=-1)
    small = jnp.pad(small, ((0, 0), (0, COLS[5] - small.shape[-1])))
    parts = tuple(g.reshape(SHARDS, -1, g.shape[-1]) for g in (grad_w_qkv, grad_w_out, grad_w_gate, grad_w_up, grad_w_down, small))
    return grad_x_emb, parts


def solution(mesh):
    row_spec = P(AXIS_NAME, None)
    vec_spec = P(AXIS_NAME)
    full_spec = P(None)
    batch_spec = P(AXIS_NAME, None, None)
    weight_specs = (vec_spec, row_spec, row_spec, row_spec, full_spec, full_spec, row_spec, vec_spec, row_spec, row_spec, row_spec)

    def device_step(tokens, positions, table_shard, attn_norm, w_query, w_key, w_value, q_norm, k_norm, w_out, mlp_norm, w_gate, w_up, w_down, dy_out):
        batch_len, seq_len = tokens.shape
        me = lax.axis_index(AXIS_NAME)
        tok = tokens.reshape(-1)
        place, ids, count, first = sort_by_owner(tok)
        meta = lax.all_gather(jnp.concatenate([tok, ids, count, first, jnp.zeros((TOKS - 2 * SHARDS,), jnp.int32)]), AXIS_NAME)
        local = meta[:, :TOKS].reshape(-1) - me * ROWS_TABLE
        where = jnp.where((local >= 0) & (local < ROWS_TABLE), local, ROWS_TABLE)
        all_ids = meta[:, TOKS:2 * TOKS].reshape(-1)
        mine = lax.dynamic_index_in_dim(meta[:, 2 * TOKS:2 * TOKS + 2 * SHARDS].reshape(SHARDS, 2, SHARDS), me, 2, keepdims=False)
        sent, sent_first = mine[:, 0], mine[:, 1]
        spread_m = spread_matrix()
        table_rows = jnp.pad(table_shard, ((0, UNROLL), (0, DP - D))).reshape(ROWS_TABLE + UNROLL, 8, 128)
        pad_rows = ((0, SUBP - SUB), (0, 0))
        sh_qkv = merge_groups(w_query, w_key, w_value, jnp.stack([attn_norm, mlp_norm], axis=-1))
        shards = [jnp.pad(w, pad_rows) for w in (sh_qkv, spread(w_out, spread_m), w_gate, w_up)]
        *full, got = front(where, table_rows, (*shards, spread(w_down, spread_m)))
        f_qkv, f_out, f_gate, f_up, f_down = (w.reshape(-1, w.shape[-1]) for w in full)
        spare = GROUP_IN - HEAD
        weights = (f_qkv[:, spare], f_qkv, q_norm, k_norm, f_out, f_qkv[:, spare + 1], f_gate, f_up, f_down)
        layer_out, saved_acts = layer_fwd(spread(got.reshape(batch_len, seq_len, DP)[..., :D], spread_m), positions, weights)
        layer_out = gather_back(layer_out, spread_m)
        grad_x_emb, parts = layer_bwd(spread(dy_out, spread_m), saved_acts, weights)
        grad_rows = grad_x_emb.reshape(TOKS, 8, 128)
        grad_rows = order_rows(place, grad_rows)
        r_qkv, r_out, r_gate, r_up, r_down, r_small = scatter_grads(parts)
        back = gather_rows(grad_rows)
        d_table = add_rows(all_ids, sent_first, sent, back.reshape(SHARDS * TOKS, 8, 128))
        g_query, g_key, g_value = split_groups(r_qkv[:SUB])
        g_attn, g_mlp, g_q, g_k = (r_small[:, i] for i in range(4))
        return (layer_out, d_table, g_attn[:SUB], g_query, g_key, g_value, g_q, g_k, unspread_columns(r_out[:SUB]), g_mlp[:SUB], r_gate[:SUB], r_up[:SUB], unspread_columns(r_down))

    return jax.shard_map(device_step, mesh=mesh, in_specs=(row_spec, row_spec, row_spec) + weight_specs + (batch_spec,), out_specs=(batch_spec, row_spec) + weight_specs, check_vma=False)
```

```python
import math
import jax
import jax.numpy as jnp
from jax import lax
from jax.experimental import pallas as pl
from jax.experimental.pallas import tpu as pltpu
from jax.sharding import PartitionSpec as P

NORM_EPS = 1e-6
ROPE_THETA = 1.0e6
AXIS_NAME = 'fsdp'
D = 960
DP = 1024
SHARDS = 16
SUB = 60
SUBP = 64
QKVP = 1920
FF = 2560
ROWS_FF = 160
MESH_ID = pl.DeviceIdType.MESH
BITS = {'z': 8, 'y': 4, 'x': 2, 'c': 1}
QKV_PIECES = ((0, 0, 896, 'xyz'), (0, 896, 1024, 'yzx'), (1, 0, DP, 'zxy'))
DOWN_PIECES = ((2, 0, 384, 'xyz'), (2, 384, 384, 'yzx'), (2, 768, 256, 'zxy'))
AG_PIECES = QKV_PIECES + DOWN_PIECES
UP_PIECES = tuple((a, first, count, order) for a in (0, 1) for first, count, order in ((0, 896, 'xyz'), (896, 896, 'yzx'), (1792, 768, 'zxy')))
MLP_PIECES = ((2, 0, FF, 'xyz'), (3, 0, FF, 'yzx'), (4, 0, DP, 'zxy'))
ATT_PIECES = QKV_PIECES + ((5, 0, 128, 'yzx'),)
ROW_PIECES = tuple((0, half + lo, count, order) for half in (0, 512) for lo, count, order in ((0, 176, 'xyz'), (176, 176, 'yzx'), (352, 160, 'zxy')))
ROWS = (SUBP, SUBP, SUBP, SUBP, ROWS_FF, SUBP)
COLS = (QKVP, DP, FF, FF, DP, 128)
TOKS = 1024
ROWS_TABLE = 3072
UNROLL = 8
HEADS, KV_HEADS, GROUP, HEAD, SEQ, HALF = 15, 5, 3, 64, 512, 256
GROUP_IN = 384
GROUP_OUT = 256
SCALE = HEAD ** -0.5
MIB = 1024 * 1024
*Q_LANES, K_LANES, V_LANES = (slice(h * HEAD, (h + 1) * HEAD) for h in range(GROUP + 2))
FIRST_ORDER = (3, 7, 5, 1, 2, 6, 4, 0)
ANY_SPEC = pl.BlockSpec(memory_space=pl.ANY)
VMEM_SPEC = pl.BlockSpec(memory_space=pltpu.VMEM)
FRONT = (0, 1, 4)
MIDDLE = (2, 3)
MLP = (2, 3, 4)
LAST = (0, 1, 5)
HOPS = ((0, 0), (0, 2), (0, 4), (0, 6), (1, 0), (1, 4), (2, 0))


def own_bits():
    me = lax.axis_index(AXIS_NAME)
    return {'z': me // 8, 'y': (me // 4) % 2, 'x': (me // 2) % 2, 'c': me % 2}


def device_at(bits, flips):
    total = 0
    for name, weight in BITS.items():
        total = total + ((1 - bits[name]) if name in flips else bits[name]) * weight
    return total


def flips_of(code, order):
    return ''.join(order[i] for i in range(3) if (code >> i) & 1)


def greet(bits):
    barrier = pltpu.get_barrier_semaphore()
    for name in BITS:
        pl.semaphore_signal(barrier, inc=1, device_id=(device_at(bits, name),), device_id_type=MESH_ID)
    pl.semaphore_wait(barrier, 4)


def split(refs, *counts):
    parts = []
    for count in counts:
        parts.append(refs[:count])
        refs = refs[count:]
    return (*parts, refs)


class Doubling:
    def __init__(self, bits, pieces, ins, outs, view, send_sem, recv_sem):
        self.bits, self.pieces, self.ins, self.outs, self.view = bits, pieces, ins, outs, view
        self.send_sem, self.recv_sem = send_sem, recv_sem
        self.started = []

    def copy(self, p, code, step, src_code):
        piece = self.pieces[p]
        a, order = piece[0], piece[3]
        shard = device_at(self.bits, flips_of(src_code, order))
        src = self.ins[a] if src_code == 0 else self.outs[a].at[shard]
        target = device_at(self.bits, 'c' if step == 3 else order[step])
        slot = 8 + src_code if step == 3 else code
        return pltpu.make_async_remote_copy(
            src_ref=self.view(src, piece), dst_ref=self.view(self.outs[a].at[shard], piece),
            send_sem=self.send_sem.at[p, slot], recv_sem=self.recv_sem.at[p, slot],
            device_id=(target,), device_id_type=MESH_ID)

    def begin(self, *args):
        self.copy(*args).start()
        self.started.append(args)

    def arrived(self, p, slot):
        piece = self.pieces[p]
        flips = flips_of(slot % 8, piece[3]) + ('c' if slot >= 8 else '')
        dst = self.view(self.outs[piece[0]].at[device_at(self.bits, flips)], piece)
        pltpu.make_async_remote_copy(
            src_ref=dst, dst_ref=dst, send_sem=self.send_sem.at[p, slot], recv_sem=self.recv_sem.at[p, slot],
            device_id=(device_at(self.bits, 'c'),), device_id_type=MESH_ID).wait_recv()

    def open(self):
        for step in range(3):
            for p in range(len(self.pieces)):
                self.begin(p, 1 << step, step, 0)
        for p in range(len(self.pieces)):
            self.begin(p, 0, 3, 0)

    def forward(self, code):
        top = 0 if code == 1 else (1 if code < 4 else 2)
        for p in range(len(self.pieces)):
            self.arrived(p, code)
            for step in range(top + 1, 3):
                self.begin(p, code | (1 << step), step, code)
            self.begin(p, 0, 3, code)

    def close(self):
        for code in range(8):
            for p in range(len(self.pieces)):
                self.arrived(p, 8 + code)
        for args in self.started:
            self.copy(*args).wait_send()


def columns_of(ref, piece):
    return ref.at[:, pl.ds(piece[1], piece[2])]


def rows_of(ref, piece):
    return ref.at[pl.ds(piece[1], piece[2])]


class OwnShards:
    def __init__(self, bits, ins, outs, stage, load_sem, store_sem):
        each = range(len(ins))
        self.loads = [pltpu.make_async_copy(ins[a], stage[a], load_sem.at[a]) for a in each]
        self.stores = [pltpu.make_async_copy(stage[a], outs[a].at[device_at(bits, '')], store_sem.at[a]) for a in each]

    def load(self):
        for load in self.loads:
            load.start()

    def store(self):
        for load, store in zip(self.loads, self.stores):
            load.wait()
            store.start()

    def close(self):
        for store in self.stores:
            store.wait()


class Halving:
    def __init__(self, bits, pieces, source, acc, got, send_sem, recv_sem):
        self.bits, self.pieces, self.source, self.acc, self.got = bits, pieces, source, acc, got
        self.send_sem, self.recv_sem = send_sem, recv_sem

    def cross(self, p, code):
        return pltpu.make_async_remote_copy(
            src_ref=self.source(p, code), dst_ref=self.acc[p].at[code],
            send_sem=self.send_sem.at[p, code], recv_sem=self.recv_sem.at[p, code],
            device_id=(device_at(self.bits, 'c'),), device_id_type=MESH_ID)

    def hop(self, p, step, code):
        sem = UNROLL + HOPS.index((step, code))
        return pltpu.make_async_remote_copy(
            src_ref=self.acc[p].at[code | (1 << step)], dst_ref=self.got[step][p].at[code >> (step + 1)],
            send_sem=self.send_sem.at[p, sem], recv_sem=self.recv_sem.at[p, sem],
            device_id=(device_at(self.bits, self.pieces[p][3][step]),), device_id_type=MESH_ID)

    def total(self, p, code, at, steps):
        total = self.acc[p][code, at]
        for step in steps:
            total = total + self.got[step][p][code >> (step + 1), at]
        return total

    def add(self, p, code, steps, put=None):
        for step in steps:
            self.hop(p, step, code).wait_recv()

        def chunk(i, carry):
            at = pl.ds(pl.multiple_of(i * UNROLL, UNROLL), UNROLL)
            total = self.total(p, code, at, steps)
            if put is None:
                self.acc[p][code, at] = total
            else:
                put(p, at, total)
            return carry

        lax.fori_loop(0, self.acc[p].shape[1] // UNROLL, chunk, 0)

    def first(self, n, fill):
        code = FIRST_ORDER[n]
        for p in range(len(self.pieces)):
            self.cross(p, code).wait_recv()
            fill(p, n, code)
            if code & 1:
                self.hop(p, 0, code - 1).start()

    def second(self):
        for code in (2, 6):
            for p in range(len(self.pieces)):
                self.add(p, code, (0,))
                self.hop(p, 1, code - 2).start()

    def third(self):
        for p in range(len(self.pieces)):
            self.add(p, 4, (0, 1))
            self.hop(p, 2, 0).start()

    def last(self, put):
        for p in range(len(self.pieces)):
            self.add(p, 0, (0, 1, 2), put)

    def close(self):
        for p in range(len(self.pieces)):
            for code in FIRST_ORDER:
                self.cross(p, code).wait_send()
            for step, code in HOPS:
                self.hop(p, step, code).wait_send()


class GradTree(Halving):
    def __init__(self, bits, pieces, ins, outs, scratch):
        np_ = len(pieces)
        acc, self.own, *got, marks = split(scratch, np_, np_, np_, np_, np_)
        send_sem, recv_sem, self.own_sem = marks
        self.ins, self.outs = ins, outs
        super().__init__(bits, pieces, lambda p, code: self.part(p, code, 'c'), acc, got, send_sem, recv_sem)

    def part(self, p, code, flips):
        piece = self.pieces[p]
        shard = device_at(self.bits, flips_of(code, piece[3]) + flips)
        return columns_of(self.ins[piece[0]].at[shard], piece)

    def own_copy(self, p, n):
        return pltpu.make_async_copy(self.part(p, FIRST_ORDER[n], ''), self.own[p].at[n % 2], self.own_sem.at[p, n % 2])

    def load(self):
        for p in range(len(self.pieces)):
            self.own_copy(p, 0).start()
            self.own_copy(p, 1).start()

    def open(self):
        for code in FIRST_ORDER:
            for p in range(len(self.pieces)):
                self.cross(p, code).start()

    def fill(self, p, n, code):
        self.own_copy(p, n).wait()
        acc, own = self.acc[p], self.own[p]

        def chunk(i, carry):
            at = pl.ds(pl.multiple_of(i * UNROLL, UNROLL), UNROLL)
            acc[code, at] = acc[code, at] + own[n % 2, at]
            return carry

        lax.fori_loop(0, acc.shape[1] // UNROLL, chunk, 0)
        if n + 2 < len(FIRST_ORDER):
            self.own_copy(p, n + 2).start()

    def put(self, p, at, total):
        a, first, cols, order = self.pieces[p]
        self.outs[a][at, pl.ds(first, cols)] = total


def tree_scratch(pieces):
    scratch = []
    for lead in (8, 2, 4, 2, 1):
        scratch += [pltpu.VMEM((lead, ROWS[piece[0]], piece[2]), jnp.float32) for piece in pieces]
    return scratch + sems(len(pieces)) + [pltpu.SemaphoreType.DMA((len(pieces), 2))]


def grad_shape(a):
    return jax.ShapeDtypeStruct((ROWS[a], COLS[a]), jnp.float32)


def columns_of(ref, piece):
    return ref.at[:, pl.ds(piece[1], piece[2])]


def rows_of(ref, piece):
    return ref.at[pl.ds(piece[1], piece[2])]


def sems(count):
    return [pltpu.SemaphoreType.DMA((count, 16))] * 2


def cost(gflops):
    return pl.CostEstimate(flops=gflops * 10 ** 9, bytes_accessed=10 ** 8, transcendentals=0)


def front_body(*refs):
    num = len(FRONT)
    np_ = len(ROW_PIECES)
    where_ref, table_ref, *refs = refs
    ins, outs, (x_ref,), stage, away, acc, *got, marks = split(refs, num, num, 1, num, np_, np_, np_, np_, np_)
    w_send, w_recv, load_sem, store_sem, x_send, x_recv = marks
    bits = own_bits()
    pieces = range(np_)
    shards = OwnShards(bits, ins, outs, stage, load_sem, store_sem)
    shards.load()
    greet(bits)
    ring = Doubling(bits, AG_PIECES, ins, outs, columns_of, w_send, w_recv)
    ring.open()
    tree = Halving(bits, ROW_PIECES, lambda p, code: away[p].at[code], acc, got, x_send, x_recv)

    def pick(p, code, other):
        first, count, order = ROW_PIECES[p][1:]
        base = device_at(bits, flips_of(code, order) + ('c' if other else '')) * TOKS + first

        def step(i, carry):
            for k in range(UNROLL):
                t = i * UNROLL + k
                row = table_ref[where_ref[base + t]]
                if other:
                    away[p][code, t] = row
                else:
                    acc[p][code, t] = acc[p][code, t] + row
            return carry

        lax.fori_loop(0, count // UNROLL, step, 0)

    for code in FIRST_ORDER:
        for p in pieces:
            pick(p, code, True)
            tree.cross(p, code).start()
    shards.store()
    for code in range(1, 4):
        ring.forward(code)
    for n in range(len(FIRST_ORDER)):
        tree.first(n, lambda p, n, code: pick(p, code, False))
    for code in range(4, UNROLL):
        ring.forward(code)

    def put(p, at, total):
        x_ref[pl.ds(ROW_PIECES[p][1] + at.start, UNROLL)] = total

    tree.second()
    tree.third()
    tree.last(put)
    tree.close()
    ring.close()
    shards.close()


def gathered_shape(a):
    return jax.ShapeDtypeStruct((SHARDS, ROWS[a], COLS[a]), jnp.bfloat16)


def shard_scratch(arrays, count):
    stage = [pltpu.VMEM((ROWS[a], COLS[a]), jnp.bfloat16) for a in arrays]
    return stage, sems(count) + [pltpu.SemaphoreType.DMA((len(arrays),))] * 2


def comm(collective_id, mib):
    return pltpu.CompilerParams(collective_id=collective_id, has_side_effects=True, vmem_limit_bytes=mib * MIB)


def front(where, table, shards):
    num = len(shards)
    scratch, marks = shard_scratch(FRONT, len(AG_PIECES))
    for lead in (8, 8, 4, 2, 1):
        scratch += [pltpu.VMEM((lead, piece[2], 8, 128), jnp.bfloat16) for piece in ROW_PIECES]
    return pl.pallas_call(
        front_body,
        out_shape=tuple(gathered_shape(a) for a in FRONT) + (jax.ShapeDtypeStruct((TOKS, 8, 128), jnp.bfloat16),),
        in_specs=[pl.BlockSpec(memory_space=pltpu.SMEM), VMEM_SPEC] + [ANY_SPEC] * num,
        out_specs=(ANY_SPEC,) * num + (VMEM_SPEC,),
        scratch_shapes=scratch + marks + sems(len(ROW_PIECES)),
        compiler_params=comm(1, 63),
        cost_estimate=cost(60),
        name='front',
    )(where, table, *shards)


def back_body(rows_ref, qkv_ref, out_ref, small_ref, all_ref, *rest):
    results, (stage, send_sem, recv_sem, own_sem), scratch = split(rest, 3, 4)
    bits = own_bits()
    load = pltpu.make_async_copy(rows_ref, stage, own_sem.at[0])
    load.start()
    tree = GradTree(bits, ATT_PIECES, dict(zip(LAST, (qkv_ref, out_ref, small_ref))), dict(zip(LAST, results)), scratch)
    tree.load()
    greet(bits)
    ring = Doubling(bits, ROW_PIECES, (rows_ref,), (all_ref,), rows_of, send_sem, recv_sem)
    tree.open()
    ring.open()
    load.wait()
    store = pltpu.make_async_copy(stage, all_ref.at[device_at(bits, '')], own_sem.at[1])
    store.start()
    for n in range(len(FIRST_ORDER)):
        tree.first(n, tree.fill)
    ring.forward(1)
    tree.second()
    ring.forward(2)
    ring.forward(3)
    tree.third()
    ring.forward(4)
    tree.last(tree.put)
    for code in range(5, UNROLL):
        ring.forward(code)
    tree.close()
    ring.close()
    store.wait()


def back(rows, *grads):
    return pl.pallas_call(
        back_body,
        out_shape=(jax.ShapeDtypeStruct((SHARDS, TOKS, 8, 128), jnp.float32), *(grad_shape(a) for a in LAST)),
        in_specs=[ANY_SPEC] * 4,
        out_specs=(ANY_SPEC,) + (VMEM_SPEC,) * 3,
        scratch_shapes=[pltpu.VMEM((TOKS, 8, 128), jnp.float32)] + sems(len(ROW_PIECES)) + [pltpu.SemaphoreType.DMA((2,))] + tree_scratch(ATT_PIECES),
        compiler_params=comm(3, 40),
        cost_estimate=cost(80),
        name='back',
    )(rows, *grads)


def spread_matrix():
    src = lax.broadcasted_iota(jnp.int32, (D, DP), 0)
    dst = lax.broadcasted_iota(jnp.int32, (D, DP), 1)
    return ((src // SUB) * SUBP + src % SUB == dst).astype(jnp.bfloat16)


def heads_matrix():
    src = lax.broadcasted_iota(jnp.int32, (KV_HEADS * GROUP_OUT, DP), 0)
    dst = lax.broadcasted_iota(jnp.int32, (KV_HEADS * GROUP_OUT, DP), 1)
    lane = src % GROUP_OUT
    feature = (src // GROUP_OUT) * GROUP * HEAD + lane
    return ((lane < GROUP * HEAD) & ((feature // SUB) * SUBP + feature % SUB == dst)).astype(jnp.bfloat16)


def matmul(spec, lhs, rhs):
    return jnp.einsum(spec, lhs, rhs, preferred_element_type=jnp.float32)


def spread(values, matrix):
    return matmul('...d,de->...e', values, matrix).astype(jnp.bfloat16)


def gather_back(values, matrix):
    return matmul('...e,de->...d', values, matrix).astype(jnp.bfloat16)


def unspread_columns(values):
    rows = values.shape[0]
    return values.reshape(rows, SHARDS, SUBP)[:, :, :SUB].reshape(rows, D)


def merge_groups(w_query, w_key, w_value, gains):
    parts = []
    for g in range(KV_HEADS):
        at = slice(g * HEAD, (g + 1) * HEAD)
        spare = jnp.pad(gains if g == 0 else gains[:, :0], ((0, 0), (0, HEAD - (2 if g == 0 else 0))))
        parts += [w_query[:, g * GROUP * HEAD:(g + 1) * GROUP * HEAD], w_key[:, at], w_value[:, at], spare]
    return jnp.concatenate(parts, axis=1)


def split_groups(merged):
    grouped = merged.reshape(merged.shape[0], KV_HEADS, GROUP_IN)
    edges = (0, GROUP * HEAD, (GROUP + 1) * HEAD, (GROUP + 2) * HEAD)
    return tuple(grouped[:, :, lo:hi].reshape(merged.shape[0], -1) for lo, hi in zip(edges, edges[1:]))


def sort_by_id(tok):
    row = lax.broadcasted_iota(jnp.int32, (TOKS, TOKS), 0)
    col = lax.broadcasted_iota(jnp.int32, (TOKS, TOKS), 1)
    ahead = (tok[None, :] < tok[:, None]) | ((tok[None, :] == tok[:, None]) & (col < row))
    place = jnp.sum(ahead.astype(jnp.int32), axis=1)
    edge = (jnp.arange(SHARDS, dtype=jnp.int32) * ROWS_TABLE)[:, None]
    below = tok[None, :] < edge
    first = jnp.sum(below.astype(jnp.int32), axis=1)
    count = jnp.sum(((tok[None, :] < edge + ROWS_TABLE) & ~below).astype(jnp.int32), axis=1)
    local = tok % ROWS_TABLE
    halves = jnp.stack([local // HEAD, local % HEAD], axis=-1).astype(jnp.bfloat16)
    halves = matmul('st,tk->sk', (row == place[None, :]).astype(jnp.bfloat16), halves).astype(jnp.int32)
    return place, halves[:, 0] * HEAD + halves[:, 1], count, first


def order_body(place_ref, in_ref, out_ref):
    def step(i, carry):
        for k in range(UNROLL):
            t = i * UNROLL + k
            out_ref[place_ref[t]] = in_ref[t]
        return carry

    lax.fori_loop(0, TOKS // UNROLL, step, 0)


def order_rows(place, rows):
    whole = pl.BlockSpec((TOKS, 8, 128), lambda i, *_: (0, 0, 0))
    return pl.pallas_call(
        order_body,
        grid_spec=pltpu.PrefetchScalarGridSpec(num_scalar_prefetch=1, grid=(1,), in_specs=[whole], out_specs=whole),
        out_shape=jax.ShapeDtypeStruct((TOKS, 8, 128), jnp.float32),
        compiler_params=pltpu.CompilerParams(vmem_limit_bytes=40 * MIB),
        name='order_rows',
    )(place, rows)


def add_body(ids_ref, first_ref, count_ref, in_ref, out_ref, acc):
    j = pl.program_id(0)
    first = first_ref[j]
    count = count_ref[j]

    @pl.when(j == 0)
    def _():
        def clear(i, carry):
            acc[pl.ds(i * UNROLL, UNROLL)] = jnp.zeros((UNROLL, 8, 128), jnp.float32)
            return carry

        lax.fori_loop(0, ROWS_TABLE // UNROLL, clear, 0)

    def add(start, num):
        ids = [ids_ref[j * TOKS + start + k] for k in range(num)]
        olds = [acc[r] for r in ids]
        total = None
        totals = []
        for k in range(num):
            base = olds[k] if k == 0 else jnp.where(ids[k] == ids[k - 1], total, olds[k])
            total = base + in_ref[start + k]
            totals.append(total)
        for r, total in zip(ids, totals):
            acc[r] = total

    def step(i, carry):
        add(first + i * UNROLL, UNROLL)
        return carry

    def tail(i, carry):
        add(first + i, 1)
        return carry

    groups = count // UNROLL
    lax.fori_loop(0, groups, step, 0)
    lax.fori_loop(groups * UNROLL, count, tail, 0)

    @pl.when(j == SHARDS - 1)
    def _():
        def flush(i, carry):
            at = pl.ds(pl.multiple_of(i * 128, 128), 128)
            for k in range(UNROLL):
                block = acc[at, k, :].T
                for half in range(2):
                    out_ref[pl.ds((2 * k + half) * SUB, SUB), at] = block[half * SUBP:half * SUBP + SUB]
            return carry

        lax.fori_loop(0, ROWS_TABLE // 128, flush, 0)


def add_rows(ids, first, count, rows):
    return pl.pallas_call(
        add_body,
        grid_spec=pltpu.PrefetchScalarGridSpec(
            num_scalar_prefetch=3, grid=(SHARDS,),
            in_specs=[pl.BlockSpec((TOKS, 8, 128), lambda j, *_: (j, 0, 0))],
            out_specs=pl.BlockSpec((D, ROWS_TABLE), lambda j, *_: (0, 0)),
            scratch_shapes=[pltpu.VMEM((ROWS_TABLE, 8, 128), jnp.float32)]),
        out_shape=jax.ShapeDtypeStruct((D, ROWS_TABLE), jnp.float32),
        compiler_params=pltpu.CompilerParams(vmem_limit_bytes=60 * MIB),
        name='add_rows',
    )(ids, first, count, rows)


def rope_tables(positions):
    half_dim = HEAD // 2
    inv_freq = jnp.exp(jnp.arange(half_dim, dtype=jnp.float32) * (-2.0 * math.log(ROPE_THETA) / HEAD))
    angles = positions.astype(jnp.float32)[:, :, None] * inv_freq
    cos_t, sin_t = jnp.cos(angles), jnp.sin(angles)
    return jnp.concatenate([cos_t, cos_t], axis=-1), jnp.concatenate([-sin_t, sin_t], axis=-1)


def swap_halves(values):
    half_dim = HEAD // 2
    return jnp.concatenate([values[:, half_dim:], values[:, :half_dim]], axis=-1)


def norm_fwd(values, width=HEAD):
    values_f = values.astype(jnp.float32)
    inv_rms = lax.rsqrt(jnp.sum(values_f * values_f, axis=-1, keepdims=True) * (1.0 / width) + NORM_EPS)
    return values_f * inv_rms, inv_rms


def norm_bwd(grad_out, normed, inv_rms, norm_gain, width=HEAD):
    grad_normed = grad_out * norm_gain.astype(jnp.float32)
    mean_term = jnp.sum(grad_normed * normed, axis=-1, keepdims=True) * (1.0 / width)
    return inv_rms * (grad_normed - normed * mean_term)


def rope_fwd(normed, gain, cos_w, sin_w):
    scaled = normed * gain
    return (scaled * cos_w + swap_halves(scaled) * sin_w).astype(jnp.bfloat16)


def dot_nt(lhs, rhs):
    return lax.dot_general(lhs, rhs, (((1,), (1,)), ((), ())), preferred_element_type=jnp.float32)


def dot_nn(lhs, rhs):
    return lax.dot_general(lhs, rhs, (((1,), (0,)), ((), ())), preferred_element_type=jnp.float32)


def dot_tn(lhs, rhs):
    return lax.dot_general(lhs, rhs, (((0,), (0,)), ((), ())), preferred_element_type=jnp.float32)


def mask_last(scores, axis):
    split = scores.shape[axis] - HALF
    key = lax.broadcasted_iota(jnp.int32, (HALF, HALF), axis)
    query = lax.broadcasted_iota(jnp.int32, (HALF, HALF), 1 - axis)
    last = jnp.where(key <= query, lax.slice_in_dim(scores, split, split + HALF, axis=axis), -1e30)
    if split == 0:
        return last
    return jnp.concatenate([lax.slice_in_dim(scores, 0, split, axis=axis), last], axis=axis)


def softmax_of(scores, axis):
    scores = mask_last(scores, axis)
    weights = jnp.exp(scores - jnp.max(scores, axis=axis, keepdims=True))
    return weights * (1.0 / jnp.sum(weights, axis=axis, keepdims=True))


def attn_fwd_unit(b, g, qkv_ref, cos_ref, sin_ref, gq_ref, gk_ref, o_ref, block):
    cos_w, sin_w = cos_ref[b], sin_ref[b]
    lanes_out = pl.ds(pl.multiple_of(g * GROUP_OUT, 128), GROUP_OUT)
    all_heads = qkv_ref[b, :, pl.ds(pl.multiple_of(g * GROUP_IN, 128), GROUP_IN)]
    k_rot = rope_fwd(norm_fwd(all_heads[:, K_LANES])[0], gk_ref[...], cos_w, sin_w)
    v_raw = all_heads[:, V_LANES]
    for r in range(GROUP):
        q_rot = rope_fwd(norm_fwd(all_heads[:, Q_LANES[r]])[0], gq_ref[...], cos_w, sin_w) * SCALE
        for lo in range(0, SEQ, HALF):
            hi = lo + HALF
            probs = softmax_of(dot_nt(k_rot[:hi], q_rot[lo:hi]), 0)
            block[lo:hi, Q_LANES[r]] = dot_tn(probs.astype(jnp.bfloat16), v_raw[:hi]).astype(jnp.bfloat16)
    block[:, K_LANES] = jnp.zeros((SEQ, HEAD), jnp.bfloat16)
    o_ref[b, :, lanes_out] = block[...]


def attn_fwd_body(*refs):
    num = len(MIDDLE)
    ins, shard_refs, (o_ref,), full_refs, (block,), stage, marks = split(refs, 5, num, 1, num, 1, num)
    w_send, w_recv, load_sem, store_sem = marks
    bits = own_bits()
    shards = OwnShards(bits, shard_refs, full_refs, stage, load_sem, store_sem)
    shards.load()
    greet(bits)
    ring = Doubling(bits, UP_PIECES, shard_refs, full_refs, columns_of, w_send, w_recv)
    ring.open()
    shards.store()

    def unit(i, carry):
        attn_fwd_unit(i // KV_HEADS, i % KV_HEADS, *ins, o_ref, block)
        for code in range(1, 5):
            @pl.when(i == 2 * code - 1)
            def _(code=code):
                ring.forward(code)

        return carry

    lax.fori_loop(0, ins[0].shape[0] * KV_HEADS, unit, 0)
    for code in range(5, UNROLL):
        ring.forward(code)
    ring.close()
    shards.close()


def attn_bwd_unit(b, g, qkv_ref, cos_ref, sin_ref, gq_ref, gk_ref, do_ref, d_ref, dgq_ref, dgk_ref, block, dq_acc, dk_acc, dv_acc):
    cos_w, sin_w = cos_ref[b], sin_ref[b]
    gain_q, gain_k = gq_ref[...], gk_ref[...]
    lanes_in = pl.ds(pl.multiple_of(g * GROUP_IN, 128), GROUP_IN)
    lanes_out = pl.ds(pl.multiple_of(g * GROUP_OUT, 128), GROUP_OUT)
    block[...] = qkv_ref[b, :, lanes_in]
    k_normed, k_inv = norm_fwd(block[:, K_LANES])
    k_rot = rope_fwd(k_normed, gain_k, cos_w, sin_w)
    k_scaled = k_rot * SCALE
    v_raw = block[:, V_LANES]
    all_grads = do_ref[b, :, lanes_out]
    dk_acc[...] = jnp.zeros_like(dk_acc)
    dv_acc[...] = jnp.zeros_like(dv_acc)
    gain_total = jnp.zeros((1, HEAD), jnp.float32)
    for r in range(GROUP):
        q_normed, q_inv = norm_fwd(block[:, Q_LANES[r]])
        q_rot = rope_fwd(q_normed, gain_q, cos_w, sin_w) * SCALE
        head_grad = all_grads[:, Q_LANES[r]]
        for lo in range(0, SEQ, HALF):
            hi = lo + HALF
            out_grad = head_grad[lo:hi]
            q_part = q_rot[lo:hi]
            probs = softmax_of(dot_nt(k_rot[:hi], q_part), 0)
            grad_probs = dot_nt(v_raw[:hi], out_grad)
            dv_acc[:hi] += dot_nn(probs.astype(jnp.bfloat16), out_grad)
            delta = jnp.sum(grad_probs * probs, axis=0, keepdims=True)
            grad_scores = (probs * (grad_probs - delta)).astype(jnp.bfloat16)
            dk_acc[:hi] += dot_nn(grad_scores, q_part)
            dq_acc[lo:hi] = dot_tn(grad_scores, k_scaled[:hi])
        grad_q = dq_acc[...]
        grad_q = grad_q * cos_w - swap_halves(grad_q) * sin_w
        gain_total = gain_total + jnp.sum(grad_q * q_normed, axis=0, keepdims=True)
        block[:, Q_LANES[r]] = norm_bwd(grad_q, q_normed, q_inv, gain_q).astype(jnp.bfloat16)
    grad_k = dk_acc[...]
    grad_k = grad_k * cos_w - swap_halves(grad_k) * sin_w
    dgq_ref[...] += gain_total
    dgk_ref[...] += jnp.sum(grad_k * k_normed, axis=0, keepdims=True)
    block[:, K_LANES] = norm_bwd(grad_k, k_normed, k_inv, gain_k).astype(jnp.bfloat16)
    block[:, V_LANES.start:] = jnp.concatenate([dv_acc[...], jnp.zeros((SEQ, HEAD), jnp.float32)], axis=-1).astype(jnp.bfloat16)
    d_ref[b, :, lanes_in] = block[...]


def attn_bwd_body(*refs):
    ins, grads, outs, results, work, scratch = split(refs, 6, 3, 3, 3, 4)
    bits = own_bits()
    tree = GradTree(bits, MLP_PIECES, dict(zip(MLP, grads)), dict(zip(MLP, results)), scratch)
    tree.load()
    for ref in outs[1:]:
        ref[...] = jnp.zeros_like(ref)
    greet(bits)
    tree.open()
    tree.first(0, tree.fill)
    tree.first(1, tree.fill)

    def unit(i, carry):
        attn_bwd_unit(i // KV_HEADS, i % KV_HEADS, *ins, *outs, *work)
        for n in range(2, len(FIRST_ORDER)):
            @pl.when(i == n // 2 - 1)
            def _(n=n):
                tree.first(n, tree.fill)

        @pl.when(i == KV_HEADS)
        def _():
            tree.second()

        return carry

    lax.fori_loop(0, ins[0].shape[0] * KV_HEADS, unit, 0)
    tree.third()
    tree.last(tree.put)
    tree.close()


def attn_fwd(qkv, tables, shards):
    stage, marks = shard_scratch(MIDDLE, len(UP_PIECES))
    return pl.pallas_call(
        attn_fwd_body,
        out_shape=(jax.ShapeDtypeStruct(qkv.shape[:2] + (KV_HEADS * GROUP_OUT,), jnp.bfloat16),) + tuple(gathered_shape(a) for a in MIDDLE),
        in_specs=[VMEM_SPEC] * (len(tables) + 1) + [ANY_SPEC] * len(shards),
        out_specs=(VMEM_SPEC,) + (ANY_SPEC,) * len(shards),
        scratch_shapes=[pltpu.VMEM((SEQ, GROUP_OUT), jnp.bfloat16)] + stage + marks,
        compiler_params=comm(4, 40),
        cost_estimate=cost(20),
        name='attn_fwd',
    )(qkv, *tables, *shards)


def attn_bwd(qkv, tables, grads):
    gain_shape = jax.ShapeDtypeStruct((1, HEAD), jnp.float32)
    return pl.pallas_call(
        attn_bwd_body,
        out_shape=(jax.ShapeDtypeStruct(qkv.shape, jnp.bfloat16), gain_shape, gain_shape, *(grad_shape(a) for a in MLP)),
        in_specs=[VMEM_SPEC] * (len(tables) + 1) + [ANY_SPEC] * len(grads),
        out_specs=(VMEM_SPEC,) * 6,
        scratch_shapes=[pltpu.VMEM((SEQ, GROUP_IN), jnp.bfloat16)] + [pltpu.VMEM((SEQ, HEAD), jnp.float32)] * 3 + tree_scratch(MLP_PIECES),
        compiler_params=comm(2, 60),
        cost_estimate=cost(60),
        name='attn_bwd',
    )(qkv, *tables, *grads)


def layer_fwd(x_emb, positions, weights, shards):
    attn_norm, w_qkv, q_norm, k_norm, w_out, mlp_norm, w_down = weights
    cos_w, sin_w = rope_tables(positions)
    gain_q = q_norm.astype(jnp.float32)[None, :]
    gain_k = k_norm.astype(jnp.float32)[None, :]
    normed1, norm1_inv = norm_fwd(x_emb, D)
    attn_in = (normed1 * attn_norm.astype(jnp.float32)).astype(jnp.bfloat16)
    attn_args = (matmul('bsd,dn->bsn', attn_in, w_qkv).astype(jnp.bfloat16), cos_w, sin_w, gain_q, gain_k)
    heads, *full = attn_fwd(attn_args[0], attn_args[1:], shards)
    w_gate, w_up = (w.reshape(-1, w.shape[-1]) for w in full)
    attn_flat = spread(heads, heads_matrix())
    hidden = (x_emb.astype(jnp.float32) + matmul('bsn,nd->bsd', attn_flat, w_out)).astype(jnp.bfloat16)
    normed2, norm2_inv = norm_fwd(hidden, D)
    mlp_in = (normed2 * mlp_norm.astype(jnp.float32)).astype(jnp.bfloat16)
    gate_pre = matmul('bsd,df->bsf', mlp_in, w_gate)
    up_proj = matmul('bsd,df->bsf', mlp_in, w_up)
    mlp_act = (jax.nn.silu(gate_pre) * up_proj).astype(jnp.bfloat16)
    layer_out = (hidden.astype(jnp.float32) + matmul('bsf,fd->bsd', mlp_act, w_down)).astype(jnp.bfloat16)
    return layer_out, (normed1, norm1_inv, attn_in, attn_args, attn_flat, normed2, norm2_inv, mlp_in, gate_pre, up_proj, mlp_act, w_gate, w_up)


def layer_bwd(dy_out, saved_acts, weights):
    attn_norm, w_qkv, q_norm, k_norm, w_out, mlp_norm, w_down = weights
    normed1, norm1_inv, attn_in, attn_args, attn_flat, normed2, norm2_inv, mlp_in, gate_pre, up_proj, mlp_act, w_gate, w_up = saved_acts
    grad_w_down = matmul('bsf,bsd->fd', mlp_act, dy_out)
    grad_act = matmul('bsd,fd->bsf', dy_out, w_down)
    gate_sig = jax.nn.sigmoid(gate_pre)
    grad_gate = (grad_act * up_proj * gate_sig * (1.0 + gate_pre * (1.0 - gate_sig))).astype(jnp.bfloat16)
    grad_up = (grad_act * gate_pre * gate_sig).astype(jnp.bfloat16)
    grad_w_gate = matmul('bsd,bsf->df', mlp_in, grad_gate)
    grad_w_up = matmul('bsd,bsf->df', mlp_in, grad_up)
    grad_mlp_in = matmul('bsf,df->bsd', grad_gate, w_gate) + matmul('bsf,df->bsd', grad_up, w_up)
    grad_mlp_norm = jnp.sum(grad_mlp_in * normed2, axis=(0, 1))
    grad_hidden = dy_out.astype(jnp.float32) + norm_bwd(grad_mlp_in, normed2, norm2_inv, mlp_norm, D)
    hidden_b = grad_hidden.astype(jnp.bfloat16)
    grad_w_out = matmul('bsn,bsd->nd', attn_flat, hidden_b)
    grad_heads = gather_back(matmul('bsd,nd->bsn', hidden_b, w_out).astype(jnp.bfloat16), heads_matrix())
    mlp_grads = [g.reshape(SHARDS, -1, g.shape[-1]) for g in (grad_w_gate, grad_w_up, grad_w_down)]
    grad_qkv, gains_q, gains_k, *mlp_shards = attn_bwd(attn_args[0], attn_args[1:] + (grad_heads,), mlp_grads)
    grad_w_qkv = matmul('bsd,bsn->dn', attn_in, grad_qkv)
    grad_attn_in = matmul('bsn,dn->bsd', grad_qkv, w_qkv)
    grad_attn_norm = jnp.sum(grad_attn_in * normed1, axis=(0, 1))
    grad_x_emb = grad_hidden + norm_bwd(grad_attn_in, normed1, norm1_inv, attn_norm, D)
    head_grads = [jnp.tile(gains[0], SHARDS) for gains in (gains_q, gains_k)]
    small = jnp.stack([grad_attn_norm, grad_mlp_norm] + head_grads, axis=-1)
    small = jnp.pad(small, ((0, 0), (0, COLS[5] - small.shape[-1])))
    parts = tuple(g.reshape(SHARDS, -1, g.shape[-1]) for g in (grad_w_qkv, grad_w_out, small))
    return grad_x_emb, parts, mlp_shards


def solution(mesh):
    row_spec = P(AXIS_NAME, None)
    vec_spec = P(AXIS_NAME)
    full_spec = P(None)
    batch_spec = P(AXIS_NAME, None, None)
    weight_specs = (vec_spec, row_spec, row_spec, row_spec, full_spec, full_spec, row_spec, vec_spec, row_spec, row_spec, row_spec)

    def device_step(tokens, positions, table_shard, attn_norm, w_query, w_key, w_value, q_norm, k_norm, w_out, mlp_norm, w_gate, w_up, w_down, dy_out):
        batch_len, seq_len = tokens.shape
        me = lax.axis_index(AXIS_NAME)
        tok = tokens.reshape(-1)
        place, ids, count, first = sort_by_id(tok)
        meta = lax.all_gather(jnp.concatenate([tok, ids, count, first, jnp.zeros((TOKS - 2 * SHARDS,), jnp.int32)]), AXIS_NAME)
        local = meta[:, :TOKS].reshape(-1) - me * ROWS_TABLE
        where = jnp.where((local >= 0) & (local < ROWS_TABLE), local, ROWS_TABLE)
        all_ids = meta[:, TOKS:2 * TOKS].reshape(-1)
        mine = lax.dynamic_index_in_dim(meta[:, 2 * TOKS:2 * TOKS + 2 * SHARDS].reshape(SHARDS, 2, SHARDS), me, 2, keepdims=False)
        sent, sent_first = mine[:, 0], mine[:, 1]
        spread_m = spread_matrix()
        table_rows = jnp.pad(table_shard, ((0, UNROLL), (0, DP - D))).reshape(ROWS_TABLE + UNROLL, 8, 128)
        pad_rows = ((0, SUBP - SUB), (0, 0))
        sh_qkv = merge_groups(w_query, w_key, w_value, jnp.stack([attn_norm, mlp_norm], axis=-1))
        *full, got = front(where, table_rows, (jnp.pad(sh_qkv, pad_rows), jnp.pad(spread(w_out, spread_m), pad_rows), spread(w_down, spread_m)))
        f_qkv, f_out, f_down = (w.reshape(-1, w.shape[-1]) for w in full)
        spare = GROUP_IN - HEAD
        weights = (f_qkv[:, spare], f_qkv, q_norm, k_norm, f_out, f_qkv[:, spare + 1], f_down)
        x_emb = spread(got.reshape(batch_len, seq_len, DP)[..., :D], spread_m)
        layer_out, saved_acts = layer_fwd(x_emb, positions, weights, [jnp.pad(w, pad_rows) for w in (w_gate, w_up)])
        layer_out = gather_back(layer_out, spread_m)
        grad_x_emb, parts, (r_gate, r_up, r_down) = layer_bwd(spread(dy_out, spread_m), saved_acts, weights)
        grad_rows = grad_x_emb.reshape(TOKS, 8, 128)
        grad_rows = order_rows(place, grad_rows)
        all_rows, r_qkv, r_out, r_small = back(grad_rows, *parts)
        d_table = add_rows(all_ids, sent_first, sent, all_rows.reshape(SHARDS * TOKS, 8, 128)).T
        g_query, g_key, g_value = split_groups(r_qkv[:SUB])
        g_attn, g_mlp, g_q, g_k = (r_small[:, i] for i in range(4))
        return (layer_out, d_table, g_attn[:SUB], g_query, g_key, g_value, g_q, g_k, unspread_columns(r_out[:SUB]), g_mlp[:SUB], r_gate[:SUB], r_up[:SUB], unspread_columns(r_down))

    return jax.shard_map(device_step, mesh=mesh, in_specs=(row_spec, row_spec, row_spec) + weight_specs + (batch_spec,), out_specs=(batch_spec, row_spec) + weight_specs, check_vma=False)
```

```python
import math
import jax
import jax.numpy as jnp
from jax import lax
from jax.experimental import pallas as pl
from jax.experimental.pallas import tpu as pltpu
from jax.sharding import PartitionSpec as P

NORM_EPS = 1e-6
ROPE_THETA = 1.0e6
AXIS_NAME = 'fsdp'
D = 960
DP = 1024
SHARDS = 16
SUB = 60
SUBP = 64
QKVP = 1920
FF = 2560
ROWS_FF = 160
MESH_ID = pl.DeviceIdType.MESH
BITS = {'z': 8, 'y': 4, 'x': 2, 'c': 1}
QKV_PIECES = ((0, 0, 896, 'xyz'), (0, 896, 1024, 'yzx'), (1, 0, DP, 'zxy'))
DOWN_PIECES = ((2, 0, 384, 'xyz'), (2, 384, 384, 'yzx'), (2, 768, 256, 'zxy'))
AG_PIECES = QKV_PIECES + DOWN_PIECES
UP_PIECES = tuple((a, first, count, order) for a in (0, 1) for first, count, order in ((0, 896, 'xyz'), (896, 896, 'yzx'), (1792, 768, 'zxy')))
MLP_PIECES = ((2, 0, FF, 'xyz'), (3, 0, FF, 'yzx'), (4, 0, DP, 'zxy'))
ATT_PIECES = QKV_PIECES + ((5, 0, 128, 'yzx'),)
ROW_PIECES = tuple((0, half + lo, count, order) for half in (0, 512) for lo, count, order in ((0, 176, 'xyz'), (176, 176, 'yzx'), (352, 160, 'zxy')))
ROWS = (SUBP, SUBP, SUBP, SUBP, ROWS_FF, SUBP)
COLS = (QKVP, DP, FF, FF, DP, 128)
TOKS = 1024
ROWS_TABLE = 3072
UNROLL = 8
LANES = 128
HEADS, KV_HEADS, GROUP, HEAD, SEQ, HALF = 15, 5, 3, 64, 512, 256
GROUP_IN = 384
GROUP_OUT = 256
SCALE = HEAD ** -0.5
MIB = 1024 * 1024
*Q_LANES, K_LANES, V_LANES = (slice(h * HEAD, (h + 1) * HEAD) for h in range(GROUP + 2))
FIRST_ORDER = (3, 7, 5, 1, 2, 6, 4, 0)
ANY_SPEC = pl.BlockSpec(memory_space=pl.ANY)
VMEM_SPEC = pl.BlockSpec(memory_space=pltpu.VMEM)
FORWARD_AT = (0, 2, 4, 5, 6, 8)
FRONT = (0, 1, 4)
MIDDLE = (2, 3)
MLP = (2, 3, 4)
LAST = (0, 1, 5)
HOPS = ((0, 0), (0, 2), (0, 4), (0, 6), (1, 0), (1, 4), (2, 0))


def own_bits():
    me = lax.axis_index(AXIS_NAME)
    return {'z': me // 8, 'y': (me // 4) % 2, 'x': (me // 2) % 2, 'c': me % 2}


def device_at(bits, flips):
    total = 0
    for name, weight in BITS.items():
        total = total + ((1 - bits[name]) if name in flips else bits[name]) * weight
    return total


def flips_of(code, order):
    return ''.join(order[i] for i in range(3) if (code >> i) & 1)


def greet(bits):
    barrier = pltpu.get_barrier_semaphore()
    for name in BITS:
        pl.semaphore_signal(barrier, inc=1, device_id=(device_at(bits, name),), device_id_type=MESH_ID)
    pl.semaphore_wait(barrier, 4)


def loop(count, body):
    lax.fori_loop(0, count, body, 0)


def split(refs, *counts):
    parts = []
    for count in counts:
        parts.append(refs[:count])
        refs = refs[count:]
    return (*parts, refs)


class Doubling:
    def __init__(self, bits, pieces, ins, outs, view, send_sem, recv_sem):
        self.bits, self.pieces, self.ins, self.outs, self.view = bits, pieces, ins, outs, view
        self.send_sem, self.recv_sem = send_sem, recv_sem
        self.started = []

    def copy(self, p, code, step, src_code):
        piece = self.pieces[p]
        a, order = piece[0], piece[3]
        shard = device_at(self.bits, flips_of(src_code, order))
        src = self.ins[a] if src_code == 0 else self.outs[a].at[shard]
        target = device_at(self.bits, 'c' if step == 3 else order[step])
        slot = 8 + src_code if step == 3 else code
        return pltpu.make_async_remote_copy(
            src_ref=self.view(src, piece), dst_ref=self.view(self.outs[a].at[shard], piece),
            send_sem=self.send_sem.at[p, slot], recv_sem=self.recv_sem.at[p, slot],
            device_id=(target,), device_id_type=MESH_ID)

    def begin(self, *args):
        self.copy(*args).start()
        self.started.append(args)

    def arrived(self, p, slot):
        piece = self.pieces[p]
        flips = flips_of(slot % 8, piece[3]) + ('c' if slot >= 8 else '')
        dst = self.view(self.outs[piece[0]].at[device_at(self.bits, flips)], piece)
        pltpu.make_async_remote_copy(
            src_ref=dst, dst_ref=dst, send_sem=self.send_sem.at[p, slot], recv_sem=self.recv_sem.at[p, slot],
            device_id=(device_at(self.bits, 'c'),), device_id_type=MESH_ID).wait_recv()

    def open(self):
        for step in range(3):
            for p in range(len(self.pieces)):
                self.begin(p, 1 << step, step, 0)
        for p in range(len(self.pieces)):
            self.begin(p, 0, 3, 0)

    def forward(self, code):
        top = 0 if code == 1 else (1 if code < 4 else 2)
        for p in range(len(self.pieces)):
            self.arrived(p, code)
            for step in range(top + 1, 3):
                self.begin(p, code | (1 << step), step, code)
            self.begin(p, 0, 3, code)

    def close(self):
        for code in range(8):
            for p in range(len(self.pieces)):
                self.arrived(p, 8 + code)
        for args in self.started:
            self.copy(*args).wait_send()


def columns_of(ref, piece):
    return ref.at[:, pl.ds(piece[1], piece[2])]


def rows_of(ref, piece):
    return ref.at[pl.ds(piece[1], piece[2])]


class OwnShards:
    def __init__(self, bits, ins, outs, stage, load_sem, store_sem):
        each = range(len(ins))
        self.loads = [pltpu.make_async_copy(ins[a], stage[a], load_sem.at[a]) for a in each]
        self.stores = [pltpu.make_async_copy(stage[a], outs[a].at[device_at(bits, '')], store_sem.at[a]) for a in each]

    def load(self):
        for load in self.loads:
            load.start()

    def store(self):
        for load, store in zip(self.loads, self.stores):
            load.wait()
            store.start()

    def close(self):
        for store in self.stores:
            store.wait()


class Halving:
    def __init__(self, bits, pieces, source, acc, got, send_sem, recv_sem):
        self.bits, self.pieces, self.source, self.acc, self.got = bits, pieces, source, acc, got
        self.send_sem, self.recv_sem = send_sem, recv_sem

    def cross(self, p, code):
        return pltpu.make_async_remote_copy(
            src_ref=self.source(p, code), dst_ref=self.acc[p].at[code],
            send_sem=self.send_sem.at[p, code], recv_sem=self.recv_sem.at[p, code],
            device_id=(device_at(self.bits, 'c'),), device_id_type=MESH_ID)

    def hop(self, p, step, code):
        sem = UNROLL + HOPS.index((step, code))
        return pltpu.make_async_remote_copy(
            src_ref=self.acc[p].at[code | (1 << step)], dst_ref=self.got[step][p].at[code >> (step + 1)],
            send_sem=self.send_sem.at[p, sem], recv_sem=self.recv_sem.at[p, sem],
            device_id=(device_at(self.bits, self.pieces[p][3][step]),), device_id_type=MESH_ID)

    def total(self, p, code, at, steps):
        total = self.acc[p][code, at]
        for step in steps:
            total = total + self.got[step][p][code >> (step + 1), at]
        return total

    def add(self, p, code, steps, put=None):
        for step in steps:
            self.hop(p, step, code).wait_recv()

        def chunk(i, carry):
            at = pl.ds(pl.multiple_of(i * UNROLL, UNROLL), UNROLL)
            total = self.total(p, code, at, steps)
            if put is None:
                self.acc[p][code, at] = total
            else:
                put(p, at, total)
            return carry

        loop(self.acc[p].shape[1] // UNROLL, chunk)

    def first(self, n, fill):
        code = FIRST_ORDER[n]
        for p in range(len(self.pieces)):
            self.cross(p, code).wait_recv()
            fill(p, n, code)
            if code & 1:
                self.hop(p, 0, code - 1).start()

    def second(self):
        for code in (2, 6):
            for p in range(len(self.pieces)):
                self.add(p, code, (0,))
                self.hop(p, 1, code - 2).start()

    def third(self):
        for p in range(len(self.pieces)):
            self.add(p, 4, (0, 1))
            self.hop(p, 2, 0).start()

    def last(self, put):
        for p in range(len(self.pieces)):
            self.add(p, 0, (0, 1, 2), put)

    def close(self):
        for p in range(len(self.pieces)):
            for code in FIRST_ORDER:
                self.cross(p, code).wait_send()
            for step, code in HOPS:
                self.hop(p, step, code).wait_send()


class GradTree(Halving):
    def __init__(self, bits, pieces, ins, outs, scratch):
        np_ = len(pieces)
        acc, self.own, *got, marks = split(scratch, np_, np_, np_, np_, np_)
        send_sem, recv_sem, self.own_sem = marks
        self.ins, self.outs = ins, outs
        super().__init__(bits, pieces, lambda p, code: self.part(p, code, 'c'), acc, got, send_sem, recv_sem)

    def part(self, p, code, flips):
        piece = self.pieces[p]
        shard = device_at(self.bits, flips_of(code, piece[3]) + flips)
        return columns_of(self.ins[piece[0]].at[shard], piece)

    def own_copy(self, p, n):
        return pltpu.make_async_copy(self.part(p, FIRST_ORDER[n], ''), self.own[p].at[n % 2], self.own_sem.at[p, n % 2])

    def load(self):
        for p in range(len(self.pieces)):
            self.own_copy(p, 0).start()
            self.own_copy(p, 1).start()

    def open(self):
        for code in FIRST_ORDER:
            for p in range(len(self.pieces)):
                self.cross(p, code).start()

    def fill(self, p, n, code):
        self.own_copy(p, n).wait()
        acc, own = self.acc[p], self.own[p]

        def chunk(i, carry):
            at = pl.ds(pl.multiple_of(i * UNROLL, UNROLL), UNROLL)
            acc[code, at] = acc[code, at] + own[n % 2, at]
            return carry

        loop(acc.shape[1] // UNROLL, chunk)
        if n + 2 < len(FIRST_ORDER):
            self.own_copy(p, n + 2).start()

    def put(self, p, at, total):
        a, first, cols, order = self.pieces[p]
        self.outs[a][at, pl.ds(first, cols)] = total


def tree_scratch(pieces):
    scratch = []
    for lead in (8, 2, 4, 2, 1):
        scratch += [pltpu.VMEM((lead, ROWS[piece[0]], piece[2]), jnp.float32) for piece in pieces]
    return scratch + sems(len(pieces)) + [pltpu.SemaphoreType.DMA((len(pieces), 2))]


def grad_shape(a):
    return jax.ShapeDtypeStruct((ROWS[a], COLS[a]), jnp.float32)


def columns_of(ref, piece):
    return ref.at[:, pl.ds(piece[1], piece[2])]


def rows_of(ref, piece):
    return ref.at[pl.ds(piece[1], piece[2])]


def sems(count):
    return [pltpu.SemaphoreType.DMA((count, 16))] * 2


def cost(gflops):
    return pl.CostEstimate(flops=gflops * 10 ** 9, bytes_accessed=10 ** 8, transcendentals=0)


def front_body(*refs):
    num = len(FRONT)
    np_ = len(ROW_PIECES)
    where_ref, table_ref, *refs = refs
    ins, outs, (x_ref,), stage, away, acc, *got, marks = split(refs, num, num, 1, num, np_, np_, np_, np_, np_)
    w_send, w_recv, load_sem, store_sem, x_send, x_recv = marks
    bits = own_bits()
    pieces = range(np_)
    shards = OwnShards(bits, ins, outs, stage, load_sem, store_sem)
    shards.load()
    greet(bits)
    ring = Doubling(bits, AG_PIECES, ins, outs, columns_of, w_send, w_recv)
    ring.open()
    tree = Halving(bits, ROW_PIECES, lambda p, code: away[p].at[code], acc, got, x_send, x_recv)

    def pick(p, code, other):
        first, count, order = ROW_PIECES[p][1:]
        base = device_at(bits, flips_of(code, order) + ('c' if other else '')) * TOKS + first

        def step(i, carry):
            for k in range(UNROLL):
                t = i * UNROLL + k
                row = table_ref[where_ref[base + t]]
                if other:
                    away[p][code, t] = row
                else:
                    acc[p][code, t] = acc[p][code, t] + row
            return carry

        loop(count // UNROLL, step)

    for code in FIRST_ORDER:
        for p in pieces:
            pick(p, code, True)
            tree.cross(p, code).start()
    shards.store()
    for code in range(1, 4):
        ring.forward(code)
    for n in range(len(FIRST_ORDER)):
        tree.first(n, lambda p, n, code: pick(p, code, False))
    for code in range(4, UNROLL):
        ring.forward(code)

    def put(p, at, total):
        x_ref[pl.ds(ROW_PIECES[p][1] + at.start, UNROLL)] = total

    tree.second()
    tree.third()
    tree.last(put)
    tree.close()
    ring.close()
    shards.close()


def gathered_shape(a):
    return jax.ShapeDtypeStruct((SHARDS, ROWS[a], COLS[a]), jnp.bfloat16)


def shard_scratch(arrays, count):
    stage = [pltpu.VMEM((ROWS[a], COLS[a]), jnp.bfloat16) for a in arrays]
    return stage, sems(count) + [pltpu.SemaphoreType.DMA((len(arrays),))] * 2


def comm(collective_id, mib):
    return pltpu.CompilerParams(collective_id=collective_id, has_side_effects=True, vmem_limit_bytes=mib * MIB)


def front(where, table, shards):
    num = len(shards)
    scratch, marks = shard_scratch(FRONT, len(AG_PIECES))
    for lead in (8, 8, 4, 2, 1):
        scratch += [pltpu.VMEM((lead, piece[2], UNROLL, LANES), jnp.bfloat16) for piece in ROW_PIECES]
    return pl.pallas_call(
        front_body,
        out_shape=tuple(gathered_shape(a) for a in FRONT) + (jax.ShapeDtypeStruct((TOKS, UNROLL, LANES), jnp.bfloat16),),
        in_specs=[pl.BlockSpec(memory_space=pltpu.SMEM), VMEM_SPEC] + [ANY_SPEC] * num,
        out_specs=(ANY_SPEC,) * num + (VMEM_SPEC,),
        scratch_shapes=scratch + marks + sems(len(ROW_PIECES)),
        compiler_params=comm(1, 63),
        cost_estimate=cost(60),
        name='front',
    )(where, table, *shards)


class LastTree(GradTree):
    def multiply(self, lhs_t, rhs, away, home):
        self.lhs_t, self.rhs, self.away, self.home = lhs_t, rhs, away, home

    def mixed(self, p):
        return self.pieces[p][0] == 0

    def products(self, into, core):
        def shard_rows(code, carry):
            for p in range(len(into)):
                first, cols, order = self.pieces[p][1:]
                shard = core
                for i, name in enumerate(order):
                    flip = (code // (1 << i)) % 2
                    shard = shard + (self.bits[name] + flip - 2 * self.bits[name] * flip) * BITS[name]
                rows = pl.ds(pl.multiple_of(shard * SUBP, SUBP), SUBP)
                into[p][code] = dot_nn(self.lhs_t[rows, :], self.rhs[:, pl.ds(first, cols)])
            return carry

        loop(UNROLL, shard_rows)

    def part(self, p, code, flips):
        return self.away[p].at[code] if self.mixed(p) else super().part(p, code, flips)

    def load(self):
        for p in range(len(self.pieces)):
            if not self.mixed(p):
                self.own_copy(p, 0).start()
                self.own_copy(p, 1).start()

    def open(self):
        self.products(self.away, 1 - self.bits['c'])
        super().open()
        self.products(self.home, self.bits['c'])

    def fill(self, p, n, code):
        if not self.mixed(p):
            super().fill(p, n, code)
            return

        def chunk(i, carry):
            at = pl.ds(pl.multiple_of(i * UNROLL, UNROLL), UNROLL)
            self.acc[p][code, at] = self.acc[p][code, at] + self.home[p][code, at]
            return carry

        loop(SUBP // UNROLL, chunk)


def back_body(rows_ref, out_ref, small_ref, *refs):
    num = 6
    ins, (all_ref,), results, (y_ref,), (stage, send_sem, recv_sem, own_sem, load_sem), held, (lhs_t,), away, home, scratch = split(refs, num, 1, 3, 1, 5, num, 1, 2, 2)
    lhs, rhs, act, down, hidden, spread_m = held
    bits = own_bits()
    load = pltpu.make_async_copy(rows_ref, stage, own_sem.at[0])
    load.start()
    loads = [pltpu.make_async_copy(ins[i], held[i], load_sem.at[i]) for i in range(num)]
    for copy in loads:
        copy.start()
    tree = LastTree(bits, ATT_PIECES, dict(zip(LAST, (None, out_ref, small_ref))), dict(zip(LAST, results)), scratch)
    tree.multiply(lhs_t, rhs, away, home)
    tree.load()
    greet(bits)
    ring = Doubling(bits, ROW_PIECES, (rows_ref,), (all_ref,), rows_of, send_sem, recv_sem)
    ring.open()
    for copy in loads:
        copy.wait()

    def turn(i, carry):
        at = pl.ds(pl.multiple_of(i * LANES, LANES), LANES)
        lhs_t[at, :] = lhs[:, at].T
        return carry

    loop(DP // LANES, turn)
    tree.open()
    load.wait()
    store = pltpu.make_async_copy(stage, all_ref.at[device_at(bits, '')], own_sem.at[1])
    store.start()
    for n in range(len(FIRST_ORDER)):
        tree.first(n, tree.fill)

    blocks = SEQ // HALF

    def project(i, carry):
        tokens = pl.ds(pl.multiple_of(i * HALF, HALF), HALF)
        total = (hidden[tokens, :].astype(jnp.float32) + dot_nn(act[tokens, :], down[...])).astype(jnp.bfloat16)
        part = pl.ds(pl.multiple_of((i % blocks) * HALF, HALF), HALF)
        y_ref[i // blocks, :, part] = dot_nt(spread_m[...], total).astype(jnp.bfloat16)
        return carry

    ring.forward(1)
    tree.second()
    ring.forward(2)
    ring.forward(3)
    tree.third()
    ring.forward(4)
    loop(TOKS // HALF, project)
    tree.last(tree.put)
    for code in range(5, UNROLL):
        ring.forward(code)
    tree.close()
    ring.close()
    store.wait()


def back(*operands):
    held = operands[3:]
    scratch = [pltpu.VMEM((TOKS, UNROLL, LANES), jnp.float32)] + sems(len(ROW_PIECES)) + [pltpu.SemaphoreType.DMA((2,)), pltpu.SemaphoreType.DMA((len(held),))]
    scratch += [pltpu.VMEM(array.shape, array.dtype) for array in held]
    scratch += [pltpu.VMEM((DP, TOKS), jnp.bfloat16)]
    scratch += [pltpu.VMEM((UNROLL, SUBP, piece[2]), jnp.float32) for piece in QKV_PIECES[:2]] * 2
    return pl.pallas_call(
        back_body,
        out_shape=(jax.ShapeDtypeStruct((SHARDS, TOKS, UNROLL, LANES), jnp.float32), *(grad_shape(a) for a in LAST), jax.ShapeDtypeStruct((TOKS // SEQ, D, SEQ), jnp.bfloat16)),
        in_specs=[ANY_SPEC] * len(operands),
        out_specs=(ANY_SPEC,) + (VMEM_SPEC,) * 4,
        scratch_shapes=scratch + tree_scratch(ATT_PIECES),
        compiler_params=comm(3, 60),
        cost_estimate=cost(80),
        name='back',
    )(*operands)


def spread_matrix():
    src = lax.broadcasted_iota(jnp.int32, (D, DP), 0)
    dst = lax.broadcasted_iota(jnp.int32, (D, DP), 1)
    return ((src // SUB) * SUBP + src % SUB == dst).astype(jnp.bfloat16)


def heads_matrix():
    src = lax.broadcasted_iota(jnp.int32, (KV_HEADS * GROUP_OUT, DP), 0)
    dst = lax.broadcasted_iota(jnp.int32, (KV_HEADS * GROUP_OUT, DP), 1)
    lane = src % GROUP_OUT
    feature = (src // GROUP_OUT) * GROUP * HEAD + lane
    return ((lane < GROUP * HEAD) & ((feature // SUB) * SUBP + feature % SUB == dst)).astype(jnp.bfloat16)


def matmul(spec, lhs, rhs):
    return jnp.einsum(spec, lhs, rhs, preferred_element_type=jnp.float32)


def spread(values, matrix):
    return matmul('...d,de->...e', values, matrix).astype(jnp.bfloat16)


def gather_back(values, matrix):
    return matmul('...e,de->...d', values, matrix).astype(jnp.bfloat16)


def unspread_columns(values):
    rows = values.shape[0]
    return values.reshape(rows, SHARDS, SUBP)[:, :, :SUB].reshape(rows, D)


def merge_groups(w_query, w_key, w_value, gains):
    parts = []
    for g in range(KV_HEADS):
        at = slice(g * HEAD, (g + 1) * HEAD)
        spare = jnp.pad(gains if g == 0 else gains[:, :0], ((0, 0), (0, HEAD - (2 if g == 0 else 0))))
        parts += [w_query[:, g * GROUP * HEAD:(g + 1) * GROUP * HEAD], w_key[:, at], w_value[:, at], spare]
    return jnp.concatenate(parts, axis=1)


def split_groups(merged):
    grouped = merged.reshape(merged.shape[0], KV_HEADS, GROUP_IN)
    edges = (0, GROUP * HEAD, (GROUP + 1) * HEAD, (GROUP + 2) * HEAD)
    return tuple(grouped[:, :, lo:hi].reshape(merged.shape[0], -1) for lo, hi in zip(edges, edges[1:]))


def sort_by_id(tok):
    row = lax.broadcasted_iota(jnp.int32, (TOKS, TOKS), 0)
    col = lax.broadcasted_iota(jnp.int32, (TOKS, TOKS), 1)
    ahead = (tok[None, :] < tok[:, None]) | ((tok[None, :] == tok[:, None]) & (col < row))
    place = jnp.sum(ahead.astype(jnp.int32), axis=1)
    edge = lax.broadcasted_iota(jnp.int32, (SHARDS, 1), 0) * ROWS_TABLE
    below = tok[None, :] < edge
    first = jnp.sum(below.astype(jnp.int32), axis=1)
    count = jnp.sum(((tok[None, :] < edge + ROWS_TABLE) & ~below).astype(jnp.int32), axis=1)
    local = tok % ROWS_TABLE
    halves = jnp.stack([local // HEAD, local % HEAD], axis=-1).astype(jnp.bfloat16)
    halves = matmul('st,tk->sk', (row == place[None, :]).astype(jnp.bfloat16), halves).astype(jnp.int32)
    return place, halves[:, 0] * HEAD + halves[:, 1], count, first


def order_body(place_ref, in_ref, out_ref):
    def step(i, carry):
        for k in range(UNROLL):
            t = i * UNROLL + k
            out_ref[place_ref[t]] = in_ref[t]
        return carry

    loop(TOKS // UNROLL, step)


def order_rows(place, rows):
    whole = pl.BlockSpec((TOKS, UNROLL, LANES), lambda i, *_: (0, 0, 0))
    return pl.pallas_call(
        order_body,
        grid_spec=pltpu.PrefetchScalarGridSpec(num_scalar_prefetch=1, grid=(1,), in_specs=[whole], out_specs=whole),
        out_shape=jax.ShapeDtypeStruct((TOKS, UNROLL, LANES), jnp.float32),
        compiler_params=pltpu.CompilerParams(vmem_limit_bytes=40 * MIB),
        name='order_rows',
    )(place, rows)


def add_body(ids_ref, first_ref, count_ref, in_ref, out_ref, acc):
    j = pl.program_id(0)
    first = first_ref[j]
    count = count_ref[j]

    @pl.when(j == 0)
    def _():
        def clear(i, carry):
            acc[pl.ds(i * UNROLL, UNROLL)] = jnp.zeros((UNROLL, UNROLL, LANES), jnp.float32)
            return carry

        loop(ROWS_TABLE // UNROLL, clear)

    def add(start, num):
        ids = [ids_ref[j * TOKS + start + k] for k in range(num)]
        olds = [acc[r] for r in ids]
        total = None
        totals = []
        for k in range(num):
            base = olds[k] if k == 0 else jnp.where(ids[k] == ids[k - 1], total, olds[k])
            total = base + in_ref[start + k]
            totals.append(total)
        for r, total in zip(ids, totals):
            acc[r] = total

    def step(i, carry):
        add(first + i * UNROLL, UNROLL)
        return carry

    def tail(i, carry):
        add(first + i, 1)
        return carry

    groups = count // UNROLL
    loop(groups, step)
    lax.fori_loop(groups * UNROLL, count, tail, 0)

    @pl.when(j == SHARDS - 1)
    def _():
        def flush(i, carry):
            at = pl.ds(pl.multiple_of(i * LANES, LANES), LANES)
            for k in range(UNROLL):
                block = acc[at, k, :].T
                for half in range(2):
                    out_ref[pl.ds((2 * k + half) * SUB, SUB), at] = block[half * SUBP:][:SUB]
            return carry

        loop(ROWS_TABLE // LANES, flush)


def add_rows(ids, first, count, rows):
    return pl.pallas_call(
        add_body,
        grid_spec=pltpu.PrefetchScalarGridSpec(
            num_scalar_prefetch=3, grid=(SHARDS,),
            in_specs=[pl.BlockSpec((TOKS, UNROLL, LANES), lambda j, *_: (j, 0, 0))],
            out_specs=pl.BlockSpec((D, ROWS_TABLE), lambda j, *_: (0, 0)),
            scratch_shapes=[pltpu.VMEM((ROWS_TABLE, UNROLL, LANES), jnp.float32)]),
        out_shape=jax.ShapeDtypeStruct((D, ROWS_TABLE), jnp.float32),
        compiler_params=pltpu.CompilerParams(vmem_limit_bytes=60 * MIB),
        name='add_rows',
    )(ids, first, count, rows)


def rope_tables(positions):
    half_dim = HEAD // 2
    inv_freq = jnp.exp(jnp.arange(half_dim, dtype=jnp.float32) * (-2.0 * math.log(ROPE_THETA) / HEAD))
    angles = positions.astype(jnp.float32)[:, :, None] * inv_freq
    cos_t, sin_t = jnp.cos(angles), jnp.sin(angles)
    return jnp.concatenate([cos_t, cos_t], axis=-1), jnp.concatenate([-sin_t, sin_t], axis=-1)


def swap_halves(values):
    half_dim = HEAD // 2
    return jnp.concatenate([values[:, half_dim:], values[:, :half_dim]], axis=-1)


def norm_fwd(values, width=HEAD):
    values_f = values.astype(jnp.float32)
    inv_rms = lax.rsqrt(jnp.sum(values_f * values_f, axis=-1, keepdims=True) * (1.0 / width) + NORM_EPS)
    return values_f * inv_rms, inv_rms


def norm_bwd(grad_out, normed, inv_rms, norm_gain, width=HEAD):
    grad_normed = grad_out * norm_gain.astype(jnp.float32)
    mean_term = jnp.sum(grad_normed * normed, axis=-1, keepdims=True) * (1.0 / width)
    return inv_rms * (grad_normed - normed * mean_term)


def rope_fwd(normed, gain, cos_w, sin_w):
    scaled = normed * gain
    return (scaled * cos_w + swap_halves(scaled) * sin_w).astype(jnp.bfloat16)


def dot_nt(lhs, rhs):
    return lax.dot_general(lhs, rhs, (((1,), (1,)), ((), ())), preferred_element_type=jnp.float32)


def dot_nn(lhs, rhs):
    return lax.dot_general(lhs, rhs, (((1,), (0,)), ((), ())), preferred_element_type=jnp.float32)


def dot_tn(lhs, rhs):
    return lax.dot_general(lhs, rhs, (((0,), (0,)), ((), ())), preferred_element_type=jnp.float32)


def mask_last(scores, axis):
    split = scores.shape[axis] - HALF
    key = lax.broadcasted_iota(jnp.int32, (HALF, HALF), axis)
    query = lax.broadcasted_iota(jnp.int32, (HALF, HALF), 1 - axis)
    last = jnp.where(key <= query, lax.slice_in_dim(scores, split, split + HALF, axis=axis), -1e30)
    if split == 0:
        return last
    return jnp.concatenate([lax.slice_in_dim(scores, 0, split, axis=axis), last], axis=axis)


def softmax_of(scores, axis):
    scores = mask_last(scores, axis)
    weights = jnp.exp(scores - jnp.max(scores, axis=axis, keepdims=True))
    return weights * (1.0 / jnp.sum(weights, axis=axis, keepdims=True))


def attn_fwd_unit(b, g, qkv_ref, cos_ref, sin_ref, gq_ref, gk_ref, o_ref, block):
    cos_w, sin_w = cos_ref[b], sin_ref[b]
    lanes_out = pl.ds(pl.multiple_of(g * GROUP_OUT, LANES), GROUP_OUT)
    all_heads = qkv_ref[b, :, pl.ds(pl.multiple_of(g * GROUP_IN, LANES), GROUP_IN)]
    k_rot = rope_fwd(norm_fwd(all_heads[:, K_LANES])[0], gk_ref[...], cos_w, sin_w)
    v_raw = all_heads[:, V_LANES]
    for r in range(GROUP):
        q_rot = rope_fwd(norm_fwd(all_heads[:, Q_LANES[r]])[0], gq_ref[...], cos_w, sin_w) * SCALE
        for lo in range(0, SEQ, HALF):
            hi = lo + HALF
            probs = softmax_of(dot_nt(k_rot[:hi], q_rot[lo:hi]), 0)
            block[lo:hi, Q_LANES[r]] = dot_tn(probs.astype(jnp.bfloat16), v_raw[:hi]).astype(jnp.bfloat16)
    block[:, K_LANES] = jnp.zeros((SEQ, HEAD), jnp.bfloat16)
    o_ref[b, :, lanes_out] = block[...]


def attn_fwd_body(*refs):
    num = len(MIDDLE)
    ins, shard_refs, (o_ref,), full_refs, (block,), stage, marks = split(refs, 5, num, 1, num, 1, num)
    w_send, w_recv, load_sem, store_sem = marks
    bits = own_bits()
    shards = OwnShards(bits, shard_refs, full_refs, stage, load_sem, store_sem)
    shards.load()
    greet(bits)
    ring = Doubling(bits, UP_PIECES, shard_refs, full_refs, columns_of, w_send, w_recv)
    ring.open()
    shards.store()

    def unit(i, carry):
        attn_fwd_unit(i // KV_HEADS, i % KV_HEADS, *ins, o_ref, block)
        for code, turn in enumerate(FORWARD_AT, 1):
            @pl.when(i == turn)
            def _(code=code):
                ring.forward(code)

        return carry

    loop(ins[0].shape[0] * KV_HEADS, unit)
    ring.forward(UNROLL - 1)
    ring.close()
    shards.close()


def attn_bwd_unit(b, g, qkv_ref, cos_ref, sin_ref, gq_ref, gk_ref, do_ref, d_ref, dgq_ref, dgk_ref, block, dq_acc, dk_acc, dv_acc):
    cos_w, sin_w = cos_ref[b], sin_ref[b]
    gain_q, gain_k = gq_ref[...], gk_ref[...]
    lanes_in = pl.ds(pl.multiple_of(g * GROUP_IN, LANES), GROUP_IN)
    lanes_out = pl.ds(pl.multiple_of(g * GROUP_OUT, LANES), GROUP_OUT)
    block[...] = qkv_ref[b, :, lanes_in]
    k_normed, k_inv = norm_fwd(block[:, K_LANES])
    k_rot = rope_fwd(k_normed, gain_k, cos_w, sin_w)
    k_scaled = k_rot * SCALE
    v_raw = block[:, V_LANES]
    all_grads = do_ref[b, :, lanes_out]
    dk_acc[...] = jnp.zeros_like(dk_acc)
    dv_acc[...] = jnp.zeros_like(dv_acc)
    gain_total = jnp.zeros((1, HEAD), jnp.float32)
    for r in range(GROUP):
        q_normed, q_inv = norm_fwd(block[:, Q_LANES[r]])
        q_rot = rope_fwd(q_normed, gain_q, cos_w, sin_w) * SCALE
        head_grad = all_grads[:, Q_LANES[r]]
        for lo in range(0, SEQ, HALF):
            hi = lo + HALF
            out_grad = head_grad[lo:hi]
            q_part = q_rot[lo:hi]
            probs = softmax_of(dot_nt(k_rot[:hi], q_part), 0)
            grad_probs = dot_nt(v_raw[:hi], out_grad)
            dv_acc[:hi] += dot_nn(probs.astype(jnp.bfloat16), out_grad)
            delta = jnp.sum(grad_probs * probs, axis=0, keepdims=True)
            grad_scores = (probs * (grad_probs - delta)).astype(jnp.bfloat16)
            dk_acc[:hi] += dot_nn(grad_scores, q_part)
            dq_acc[lo:hi] = dot_tn(grad_scores, k_scaled[:hi])
        grad_q = dq_acc[...]
        grad_q = grad_q * cos_w - swap_halves(grad_q) * sin_w
        gain_total = gain_total + jnp.sum(grad_q * q_normed, axis=0, keepdims=True)
        block[:, Q_LANES[r]] = norm_bwd(grad_q, q_normed, q_inv, gain_q).astype(jnp.bfloat16)
    grad_k = dk_acc[...]
    grad_k = grad_k * cos_w - swap_halves(grad_k) * sin_w
    dgq_ref[...] += gain_total
    dgk_ref[...] += jnp.sum(grad_k * k_normed, axis=0, keepdims=True)
    block[:, K_LANES] = norm_bwd(grad_k, k_normed, k_inv, gain_k).astype(jnp.bfloat16)
    block[:, V_LANES.start:] = jnp.concatenate([dv_acc[...], jnp.zeros((SEQ, HEAD), jnp.float32)], axis=-1).astype(jnp.bfloat16)
    d_ref[b, :, lanes_in] = block[...]


def attn_bwd_body(*refs):
    ins, (w_qkv,), grads, outs, (in_grad,), results, work, scratch = split(refs, 6, 1, 3, 3, 1, 3, 4)
    bits = own_bits()
    tree = GradTree(bits, MLP_PIECES, dict(zip(MLP, grads)), dict(zip(MLP, results)), scratch)
    tree.load()
    for ref in outs[1:]:
        ref[...] = jnp.zeros_like(ref)
    greet(bits)
    tree.open()
    tree.first(0, tree.fill)
    tree.first(1, tree.fill)

    def unit(i, carry):
        attn_bwd_unit(i // KV_HEADS, i % KV_HEADS, *ins, *outs, *work)
        for n in range(2, len(FIRST_ORDER)):
            @pl.when(i == n // 2 - 1)
            def _(n=n):
                tree.first(n, tree.fill)

        @pl.when(i == KV_HEADS)
        def _():
            tree.second()

        return carry

    loop(ins[0].shape[0] * KV_HEADS, unit)
    qkv_grad, blocks = outs[0], SEQ // HALF

    def input_grad(i, carry):
        rows = pl.ds(pl.multiple_of((i % blocks) * HALF, HALF), HALF)
        in_grad[i // blocks, rows, :] = dot_nt(qkv_grad[i // blocks, rows, :], w_qkv[...])
        return carry

    loop(blocks * qkv_grad.shape[0], input_grad)
    tree.third()
    tree.last(tree.put)
    tree.close()


def attn_fwd(qkv, tables, shards):
    stage, marks = shard_scratch(MIDDLE, len(UP_PIECES))
    return pl.pallas_call(
        attn_fwd_body,
        out_shape=(jax.ShapeDtypeStruct(qkv.shape[:2] + (KV_HEADS * GROUP_OUT,), jnp.bfloat16),) + tuple(gathered_shape(a) for a in MIDDLE),
        in_specs=[VMEM_SPEC] * (len(tables) + 1) + [ANY_SPEC] * len(shards),
        out_specs=(VMEM_SPEC,) + (ANY_SPEC,) * len(shards),
        scratch_shapes=[pltpu.VMEM((SEQ, GROUP_OUT), jnp.bfloat16)] + stage + marks,
        compiler_params=comm(4, 40),
        cost_estimate=cost(20),
        name='attn_fwd',
    )(qkv, *tables, *shards)


def attn_bwd(qkv, tables, w_qkv, grads):
    gain_shape = jax.ShapeDtypeStruct((1, HEAD), jnp.float32)
    return pl.pallas_call(
        attn_bwd_body,
        out_shape=(jax.ShapeDtypeStruct(qkv.shape, jnp.bfloat16), gain_shape, gain_shape, jax.ShapeDtypeStruct(qkv.shape[:2] + (DP,), jnp.float32), *(grad_shape(a) for a in MLP)),
        in_specs=[VMEM_SPEC] * (len(tables) + 2) + [ANY_SPEC] * len(grads),
        out_specs=(VMEM_SPEC,) * 7,
        scratch_shapes=[pltpu.VMEM((SEQ, GROUP_IN), jnp.bfloat16)] + [pltpu.VMEM((SEQ, HEAD), jnp.float32)] * 3 + tree_scratch(MLP_PIECES),
        compiler_params=comm(2, 63),
        cost_estimate=cost(60),
        name='attn_bwd',
    )(qkv, *tables, w_qkv, *grads)


def layer_fwd(x_emb, positions, weights, shards, dy_s):
    attn_norm, w_qkv, q_norm, k_norm, w_out, mlp_norm, w_down = weights
    cos_w, sin_w = rope_tables(positions)
    gain_q = q_norm.astype(jnp.float32)[None, :]
    gain_k = k_norm.astype(jnp.float32)[None, :]
    normed1, norm1_inv = norm_fwd(x_emb, D)
    attn_in = (normed1 * attn_norm.astype(jnp.float32)).astype(jnp.bfloat16)
    attn_args = (matmul('bsd,dn->bsn', attn_in, w_qkv).astype(jnp.bfloat16), cos_w, sin_w, gain_q, gain_k)
    heads, *full = attn_fwd(attn_args[0], attn_args[1:], shards)
    w_gate, w_up = (w.reshape(-1, w.shape[-1]) for w in full)
    attn_flat = spread(heads, heads_matrix())
    hidden = (x_emb.astype(jnp.float32) + matmul('bsn,nd->bsd', attn_flat, w_out)).astype(jnp.bfloat16)
    normed2, norm2_inv = norm_fwd(hidden, D)
    mlp_in = (normed2 * mlp_norm.astype(jnp.float32)).astype(jnp.bfloat16)
    gate_pre = matmul('bsd,df->bsf', mlp_in, w_gate)
    up_proj = matmul('bsd,df->bsf', mlp_in, w_up)
    gate_pre, up_proj, dy_s = lax.optimization_barrier((gate_pre, up_proj, dy_s))
    mlp_act = (jax.nn.silu(gate_pre) * up_proj).astype(jnp.bfloat16)
    return (mlp_act.reshape(TOKS, FF), w_down, hidden.reshape(TOKS, DP)), dy_s, (normed1, norm1_inv, attn_in, attn_args, attn_flat, normed2, norm2_inv, mlp_in, gate_pre, up_proj, mlp_act, w_gate, w_up)


def layer_bwd(dy_out, saved_acts, weights):
    attn_norm, w_qkv, q_norm, k_norm, w_out, mlp_norm, w_down = weights
    normed1, norm1_inv, attn_in, attn_args, attn_flat, normed2, norm2_inv, mlp_in, gate_pre, up_proj, mlp_act, w_gate, w_up = saved_acts
    grad_w_down = matmul('bsf,bsd->fd', mlp_act, dy_out)
    grad_act = matmul('bsd,fd->bsf', dy_out, w_down)
    gate_sig = jax.nn.sigmoid(gate_pre)
    grad_gate = (grad_act * up_proj * gate_sig * (1.0 + gate_pre * (1.0 - gate_sig))).astype(jnp.bfloat16)
    grad_up = (grad_act * gate_pre * gate_sig).astype(jnp.bfloat16)
    grad_w_gate = matmul('bsd,bsf->df', mlp_in, grad_gate)
    grad_w_up = matmul('bsd,bsf->df', mlp_in, grad_up)
    grad_mlp_in = matmul('bsf,df->bsd', grad_gate, w_gate) + matmul('bsf,df->bsd', grad_up, w_up)
    grad_mlp_norm = jnp.sum(grad_mlp_in * normed2, axis=(0, 1))
    grad_hidden = dy_out.astype(jnp.float32) + norm_bwd(grad_mlp_in, normed2, norm2_inv, mlp_norm, D)
    hidden_b = grad_hidden.astype(jnp.bfloat16)
    grad_w_out = matmul('bsn,bsd->nd', attn_flat, hidden_b)
    grad_heads = gather_back(matmul('bsd,nd->bsn', hidden_b, w_out).astype(jnp.bfloat16), heads_matrix())
    mlp_grads = [g.reshape(SHARDS, -1, g.shape[-1]) for g in (grad_w_gate, grad_w_up, grad_w_down)]
    grad_qkv, gains_q, gains_k, grad_attn_in, *mlp_shards = attn_bwd(attn_args[0], attn_args[1:] + (grad_heads,), w_qkv, mlp_grads)
    grad_attn_norm = jnp.sum(grad_attn_in * normed1, axis=(0, 1))
    grad_x_emb = grad_hidden + norm_bwd(grad_attn_in, normed1, norm1_inv, attn_norm, D)
    head_grads = [jnp.tile(gains[0], SHARDS) for gains in (gains_q, gains_k)]
    small = jnp.stack([grad_attn_norm, grad_mlp_norm] + head_grads, axis=-1)
    small = jnp.pad(small, ((0, 0), (0, COLS[5] - small.shape[-1])))
    parts = tuple(g.reshape(SHARDS, -1, g.shape[-1]) for g in (grad_w_out, small))
    return grad_x_emb, (*parts, attn_in.reshape(TOKS, DP), grad_qkv.reshape(TOKS, QKVP)), mlp_shards


def solution(mesh):
    row_spec = P(AXIS_NAME, None)
    vec_spec = P(AXIS_NAME)
    full_spec = P(None)
    batch_spec = P(AXIS_NAME, None, None)
    weight_specs = (vec_spec, row_spec, row_spec, row_spec, full_spec, full_spec, row_spec, vec_spec, row_spec, row_spec, row_spec)

    def device_step(tokens, positions, table_shard, attn_norm, w_query, w_key, w_value, q_norm, k_norm, w_out, mlp_norm, w_gate, w_up, w_down, dy_out):
        batch_len, seq_len = tokens.shape
        me = lax.axis_index(AXIS_NAME)
        tok = tokens.reshape(-1)
        place, ids, count, first = sort_by_id(tok)
        meta = lax.all_gather(jnp.concatenate([tok, ids, count, first, jnp.zeros((TOKS - 2 * SHARDS,), jnp.int32)]), AXIS_NAME)
        local = meta[:, :TOKS].reshape(-1) - me * ROWS_TABLE
        where = jnp.where((local >= 0) & (local < ROWS_TABLE), local, ROWS_TABLE)
        all_ids = meta[:, TOKS:2 * TOKS].reshape(-1)
        mine = lax.dynamic_index_in_dim(meta[:, 2 * TOKS:2 * TOKS + 2 * SHARDS].reshape(SHARDS, 2, SHARDS), me, 2, keepdims=False)
        sent, sent_first = mine[:, 0], mine[:, 1]
        spread_m = spread_matrix()
        table_rows = jnp.pad(table_shard, ((0, UNROLL), (0, DP - D))).reshape(ROWS_TABLE + UNROLL, UNROLL, LANES)
        pad_rows = ((0, SUBP - SUB), (0, 0))
        sh_qkv = merge_groups(w_query, w_key, w_value, jnp.stack([attn_norm, mlp_norm], axis=-1))
        *full, got = front(where, table_rows, (jnp.pad(sh_qkv, pad_rows), jnp.pad(spread(w_out, spread_m), pad_rows), spread(w_down, spread_m)))
        f_qkv, f_out, f_down = (w.reshape(-1, w.shape[-1]) for w in full)
        spare = GROUP_IN - HEAD
        weights = (f_qkv[:, spare], f_qkv, q_norm, k_norm, f_out, f_qkv[:, spare + 1], f_down)
        x_emb = spread(got.reshape(batch_len, seq_len, DP)[..., :D], spread_m)
        last, dy_s, saved_acts = layer_fwd(x_emb, positions, weights, [jnp.pad(w, pad_rows) for w in (w_gate, w_up)], spread(dy_out, spread_m))
        grad_x_emb, parts, (r_gate, r_up, r_down) = layer_bwd(dy_s, saved_acts, weights)
        grad_rows = grad_x_emb.reshape(TOKS, UNROLL, LANES)
        grad_rows = order_rows(place, grad_rows)
        all_rows, r_qkv, r_out, r_small, y_t = back(grad_rows, *parts, *last, spread_m)
        layer_out = y_t.transpose(0, 2, 1)
        d_table = add_rows(all_ids, sent_first, sent, all_rows.reshape(SHARDS * TOKS, UNROLL, LANES)).T
        g_query, g_key, g_value = split_groups(r_qkv[:SUB])
        g_attn, g_mlp, g_q, g_k = (r_small[:, i] for i in range(4))
        return (layer_out, d_table, g_attn[:SUB], g_query, g_key, g_value, g_q, g_k, unspread_columns(r_out[:SUB]), g_mlp[:SUB], r_gate[:SUB], r_up[:SUB], unspread_columns(r_down))

    return jax.shard_map(device_step, mesh=mesh, in_specs=(row_spec, row_spec, row_spec) + weight_specs + (batch_spec,), out_specs=(batch_spec, row_spec) + weight_specs, check_vma=False)
```

```python
import math
import jax
import jax.numpy as jnp
from jax import lax
from jax.experimental import pallas as pl
from jax.experimental.pallas import tpu as pltpu
from jax.sharding import PartitionSpec as P

NORM_EPS = 1e-6
ROPE_THETA = 1.0e6
AXIS_NAME = 'fsdp'
D = 960
DP = 1024
SHARDS = 16
SUB = 60
SUBP = 64
QKVP = 1920
FF = 2560
ROWS_FF = 160
MESH_ID = pl.DeviceIdType.MESH
BITS = {'z': 8, 'y': 4, 'x': 2, 'c': 1}
QKV_PIECES = ((0, 0, 896, 'xyz'), (0, 896, 1024, 'yzx'), (1, 0, DP, 'zxy'))
DOWN_PIECES = ((2, 0, 384, 'xyz'), (2, 384, 384, 'yzx'), (2, 768, 256, 'zxy'))
AG_PIECES = QKV_PIECES + DOWN_PIECES
UP_PIECES = tuple((a, first, count, order) for a in (0, 1) for first, count, order in ((0, 896, 'xyz'), (896, 896, 'yzx'), (1792, 768, 'zxy')))
MLP_PIECES = ((2, 0, FF, 'xyz'), (3, 0, FF, 'yzx'), (4, 0, DP, 'zxy'))
ATT_PIECES = QKV_PIECES + ((5, 0, 128, 'yzx'),)
ROW_PIECES = tuple((0, half + lo, count, order) for half in (0, 512) for lo, count, order in ((0, 176, 'xyz'), (176, 176, 'yzx'), (352, 160, 'zxy')))
ROWS = (SUBP, SUBP, SUBP, SUBP, ROWS_FF, SUBP)
COLS = (QKVP, DP, FF, FF, DP, 128)
TOKS = 1024
ROWS_TABLE = 3072
UNROLL = 8
LANES = 128
HEADS, KV_HEADS, GROUP, HEAD, SEQ, HALF = 15, 5, 3, 64, 512, 256
GROUP_IN = 384
GROUP_OUT = 256
SCALE = HEAD ** -0.5
MIB = 1024 * 1024
*Q_LANES, K_LANES, V_LANES = (slice(h * HEAD, (h + 1) * HEAD) for h in range(GROUP + 2))
FIRST_ORDER = (3, 7, 5, 1, 2, 6, 4, 0)
ANY_SPEC = pl.BlockSpec(memory_space=pl.ANY)
VMEM_SPEC = pl.BlockSpec(memory_space=pltpu.VMEM)
FORWARD_AT = (0, 2, 4, 5, 6, 8)
FRONT = (0, 1, 4)
MIDDLE = (2, 3)
MLP = (2, 3, 4)
LAST = (0, 1, 5)
HOPS = ((0, 0), (0, 2), (0, 4), (0, 6), (1, 0), (1, 4), (2, 0))


def own_bits():
    me = lax.axis_index(AXIS_NAME)
    return {'z': me // 8, 'y': (me // 4) % 2, 'x': (me // 2) % 2, 'c': me % 2}


def device_at(bits, flips):
    total = 0
    for name, weight in BITS.items():
        total = total + ((1 - bits[name]) if name in flips else bits[name]) * weight
    return total


def flips_of(code, order):
    return ''.join(order[i] for i in range(3) if (code >> i) & 1)


def greet(bits):
    barrier = pltpu.get_barrier_semaphore()
    for name in BITS:
        pl.semaphore_signal(barrier, inc=1, device_id=(device_at(bits, name),), device_id_type=MESH_ID)
    pl.semaphore_wait(barrier, 4)


def loop(count, body):
    lax.fori_loop(0, count, body, 0)


def split(refs, *counts):
    parts = []
    for count in counts:
        parts.append(refs[:count])
        refs = refs[count:]
    return (*parts, refs)


class Doubling:
    def __init__(self, bits, pieces, ins, outs, view, send_sem, recv_sem):
        self.bits, self.pieces, self.ins, self.outs, self.view = bits, pieces, ins, outs, view
        self.send_sem, self.recv_sem = send_sem, recv_sem
        self.started = []

    def copy(self, p, code, step, src_code):
        piece = self.pieces[p]
        a, order = piece[0], piece[3]
        shard = device_at(self.bits, flips_of(src_code, order))
        src = self.ins[a] if src_code == 0 else self.outs[a].at[shard]
        target = device_at(self.bits, 'c' if step == 3 else order[step])
        slot = 8 + src_code if step == 3 else code
        return pltpu.make_async_remote_copy(
            src_ref=self.view(src, piece), dst_ref=self.view(self.outs[a].at[shard], piece),
            send_sem=self.send_sem.at[p, slot], recv_sem=self.recv_sem.at[p, slot],
            device_id=(target,), device_id_type=MESH_ID)

    def begin(self, *args):
        self.copy(*args).start()
        self.started.append(args)

    def arrived(self, p, slot):
        piece = self.pieces[p]
        flips = flips_of(slot % 8, piece[3]) + ('c' if slot >= 8 else '')
        dst = self.view(self.outs[piece[0]].at[device_at(self.bits, flips)], piece)
        pltpu.make_async_remote_copy(
            src_ref=dst, dst_ref=dst, send_sem=self.send_sem.at[p, slot], recv_sem=self.recv_sem.at[p, slot],
            device_id=(device_at(self.bits, 'c'),), device_id_type=MESH_ID).wait_recv()

    def open(self):
        for step in range(3):
            for p in range(len(self.pieces)):
                self.begin(p, 1 << step, step, 0)
        for p in range(len(self.pieces)):
            self.begin(p, 0, 3, 0)

    def forward(self, code):
        top = 0 if code == 1 else (1 if code < 4 else 2)
        for p in range(len(self.pieces)):
            self.arrived(p, code)
            for step in range(top + 1, 3):
                self.begin(p, code | (1 << step), step, code)
            self.begin(p, 0, 3, code)

    def close(self):
        for code in range(8):
            for p in range(len(self.pieces)):
                self.arrived(p, 8 + code)
        for args in self.started:
            self.copy(*args).wait_send()


def columns_of(ref, piece):
    return ref.at[:, pl.ds(piece[1], piece[2])]


def rows_of(ref, piece):
    return ref.at[pl.ds(piece[1], piece[2])]


class OwnShards:
    def __init__(self, bits, ins, outs, stage, load_sem, store_sem):
        each = range(len(ins))
        self.loads = [pltpu.make_async_copy(ins[a], stage[a], load_sem.at[a]) for a in each]
        self.stores = [pltpu.make_async_copy(stage[a], outs[a].at[device_at(bits, '')], store_sem.at[a]) for a in each]

    def load(self):
        for load in self.loads:
            load.start()

    def store(self):
        for load, store in zip(self.loads, self.stores):
            load.wait()
            store.start()

    def close(self):
        for store in self.stores:
            store.wait()


class Halving:
    def __init__(self, bits, pieces, source, acc, got, send_sem, recv_sem):
        self.bits, self.pieces, self.source, self.acc, self.got = bits, pieces, source, acc, got
        self.send_sem, self.recv_sem = send_sem, recv_sem

    def cross(self, p, code):
        return pltpu.make_async_remote_copy(
            src_ref=self.source(p, code), dst_ref=self.acc[p].at[code],
            send_sem=self.send_sem.at[p, code], recv_sem=self.recv_sem.at[p, code],
            device_id=(device_at(self.bits, 'c'),), device_id_type=MESH_ID)

    def hop(self, p, step, code):
        sem = UNROLL + HOPS.index((step, code))
        return pltpu.make_async_remote_copy(
            src_ref=self.acc[p].at[code | (1 << step)], dst_ref=self.got[step][p].at[code >> (step + 1)],
            send_sem=self.send_sem.at[p, sem], recv_sem=self.recv_sem.at[p, sem],
            device_id=(device_at(self.bits, self.pieces[p][3][step]),), device_id_type=MESH_ID)

    def total(self, p, code, at, steps):
        total = self.acc[p][code, at]
        for step in steps:
            total = total + self.got[step][p][code >> (step + 1), at]
        return total

    def add(self, p, code, steps, put=None):
        for step in steps:
            self.hop(p, step, code).wait_recv()

        def chunk(i, carry):
            at = pl.ds(pl.multiple_of(i * UNROLL, UNROLL), UNROLL)
            total = self.total(p, code, at, steps)
            if put is None:
                self.acc[p][code, at] = total
            else:
                put(p, at, total)
            return carry

        loop(self.acc[p].shape[1] // UNROLL, chunk)

    def first(self, n, fill):
        code = FIRST_ORDER[n]
        for p in range(len(self.pieces)):
            self.cross(p, code).wait_recv()
            fill(p, n, code)
            if code & 1:
                self.hop(p, 0, code - 1).start()

    def second(self):
        for code in (2, 6):
            for p in range(len(self.pieces)):
                self.add(p, code, (0,))
                self.hop(p, 1, code - 2).start()

    def third(self):
        for p in range(len(self.pieces)):
            self.add(p, 4, (0, 1))
            self.hop(p, 2, 0).start()

    def last(self, put):
        for p in range(len(self.pieces)):
            self.add(p, 0, (0, 1, 2), put)

    def close(self):
        for p in range(len(self.pieces)):
            for code in FIRST_ORDER:
                self.cross(p, code).wait_send()
            for step, code in HOPS:
                self.hop(p, step, code).wait_send()


class GradTree(Halving):
    def __init__(self, bits, pieces, ins, outs, scratch):
        np_ = len(pieces)
        acc, self.own, *got, marks = split(scratch, np_, np_, np_, np_, np_)
        send_sem, recv_sem, self.own_sem = marks
        self.ins, self.outs = ins, outs
        super().__init__(bits, pieces, lambda p, code: self.part(p, code, 'c'), acc, got, send_sem, recv_sem)

    def part(self, p, code, flips):
        piece = self.pieces[p]
        shard = device_at(self.bits, flips_of(code, piece[3]) + flips)
        return columns_of(self.ins[piece[0]].at[shard], piece)

    def own_copy(self, p, n):
        return pltpu.make_async_copy(self.part(p, FIRST_ORDER[n], ''), self.own[p].at[n % 2], self.own_sem.at[p, n % 2])

    def load(self):
        for p in range(len(self.pieces)):
            self.own_copy(p, 0).start()
            self.own_copy(p, 1).start()

    def open(self):
        for code in FIRST_ORDER:
            for p in range(len(self.pieces)):
                self.cross(p, code).start()

    def fill(self, p, n, code):
        self.own_copy(p, n).wait()
        acc, own = self.acc[p], self.own[p]

        def chunk(i, carry):
            at = pl.ds(pl.multiple_of(i * UNROLL, UNROLL), UNROLL)
            acc[code, at] = acc[code, at] + own[n % 2, at]
            return carry

        loop(acc.shape[1] // UNROLL, chunk)
        if n + 2 < len(FIRST_ORDER):
            self.own_copy(p, n + 2).start()

    def put(self, p, at, total):
        a, first, cols, order = self.pieces[p]
        self.outs[a][at, pl.ds(first, cols)] = total


def tree_scratch(pieces):
    scratch = []
    for lead in (8, 2, 4, 2, 1):
        scratch += [pltpu.VMEM((lead, ROWS[piece[0]], piece[2]), jnp.float32) for piece in pieces]
    return scratch + sems(len(pieces)) + [pltpu.SemaphoreType.DMA((len(pieces), 2))]


def grad_shape(a):
    return jax.ShapeDtypeStruct((ROWS[a], COLS[a]), jnp.float32)


def columns_of(ref, piece):
    return ref.at[:, pl.ds(piece[1], piece[2])]


def rows_of(ref, piece):
    return ref.at[pl.ds(piece[1], piece[2])]


def sems(count):
    return [pltpu.SemaphoreType.DMA((count, 16))] * 2


def cost(gflops):
    return pl.CostEstimate(flops=gflops * 10 ** 9, bytes_accessed=10 ** 8, transcendentals=0)


def front_body(*refs):
    num = len(FRONT)
    np_ = len(ROW_PIECES)
    where_ref, table_ref, *refs = refs
    ins, outs, (x_ref,), stage, away, acc, *got, marks = split(refs, num, num, 1, num, np_, np_, np_, np_, np_)
    w_send, w_recv, load_sem, store_sem, x_send, x_recv = marks
    bits = own_bits()
    pieces = range(np_)
    shards = OwnShards(bits, ins, outs, stage, load_sem, store_sem)
    shards.load()
    greet(bits)
    ring = Doubling(bits, AG_PIECES, ins, outs, columns_of, w_send, w_recv)
    ring.open()
    tree = Halving(bits, ROW_PIECES, lambda p, code: away[p].at[code], acc, got, x_send, x_recv)

    def pick(p, code, other):
        first, count, order = ROW_PIECES[p][1:]
        base = device_at(bits, flips_of(code, order) + ('c' if other else '')) * TOKS + first

        def step(i, carry):
            for k in range(UNROLL):
                t = i * UNROLL + k
                row = table_ref[where_ref[base + t]]
                if other:
                    away[p][code, t] = row
                else:
                    acc[p][code, t] = acc[p][code, t] + row
            return carry

        loop(count // UNROLL, step)

    for code in FIRST_ORDER:
        for p in pieces:
            pick(p, code, True)
            tree.cross(p, code).start()
    shards.store()
    for code in range(1, 4):
        ring.forward(code)
    for n in range(len(FIRST_ORDER)):
        tree.first(n, lambda p, n, code: pick(p, code, False))
    for code in range(4, UNROLL):
        ring.forward(code)

    def put(p, at, total):
        x_ref[pl.ds(ROW_PIECES[p][1] + at.start, UNROLL)] = total

    tree.second()
    tree.third()
    tree.last(put)
    tree.close()
    ring.close()
    shards.close()


def gathered_shape(a):
    return jax.ShapeDtypeStruct((SHARDS, ROWS[a], COLS[a]), jnp.bfloat16)


def shard_scratch(arrays, count):
    stage = [pltpu.VMEM((ROWS[a], COLS[a]), jnp.bfloat16) for a in arrays]
    return stage, sems(count) + [pltpu.SemaphoreType.DMA((len(arrays),))] * 2


def comm(collective_id, mib):
    return pltpu.CompilerParams(collective_id=collective_id, has_side_effects=True, vmem_limit_bytes=mib * MIB)


def front(where, table, shards):
    num = len(shards)
    scratch, marks = shard_scratch(FRONT, len(AG_PIECES))
    for lead in (8, 8, 4, 2, 1):
        scratch += [pltpu.VMEM((lead, piece[2], UNROLL, LANES), jnp.bfloat16) for piece in ROW_PIECES]
    return pl.pallas_call(
        front_body,
        out_shape=tuple(gathered_shape(a) for a in FRONT) + (jax.ShapeDtypeStruct((TOKS, UNROLL, LANES), jnp.bfloat16),),
        in_specs=[pl.BlockSpec(memory_space=pltpu.SMEM), VMEM_SPEC] + [ANY_SPEC] * num,
        out_specs=(ANY_SPEC,) * num + (VMEM_SPEC,),
        scratch_shapes=scratch + marks + sems(len(ROW_PIECES)),
        compiler_params=comm(1, 63),
        cost_estimate=cost(60),
        name='front',
    )(where, table, *shards)


class LastTree(GradTree):
    def multiply(self, lhs_t, rhs, away, home):
        self.lhs_t, self.rhs, self.away, self.home = lhs_t, rhs, away, home

    def mixed(self, p):
        return self.pieces[p][0] == 0

    def products(self, into, core):
        def shard_rows(code, carry):
            for p in range(len(into)):
                first, cols, order = self.pieces[p][1:]
                shard = core
                for i, name in enumerate(order):
                    flip = (code // (1 << i)) % 2
                    shard = shard + (self.bits[name] + flip - 2 * self.bits[name] * flip) * BITS[name]
                rows = pl.ds(pl.multiple_of(shard * SUBP, SUBP), SUBP)
                into[p][code] = dot_nn(self.lhs_t[rows, :], self.rhs[:, pl.ds(first, cols)])
            return carry

        loop(UNROLL, shard_rows)

    def part(self, p, code, flips):
        return self.away[p].at[code] if self.mixed(p) else super().part(p, code, flips)

    def load(self):
        for p in range(len(self.pieces)):
            if not self.mixed(p):
                self.own_copy(p, 0).start()
                self.own_copy(p, 1).start()

    def open(self):
        self.products(self.away, 1 - self.bits['c'])
        super().open()
        self.products(self.home, self.bits['c'])

    def fill(self, p, n, code):
        if not self.mixed(p):
            super().fill(p, n, code)
            return

        def chunk(i, carry):
            at = pl.ds(pl.multiple_of(i * UNROLL, UNROLL), UNROLL)
            self.acc[p][code, at] = self.acc[p][code, at] + self.home[p][code, at]
            return carry

        loop(SUBP // UNROLL, chunk)


def back_body(rows_ref, out_ref, small_ref, *refs):
    num = 6
    ins, (all_ref,), results, (y_ref,), (stage, send_sem, recv_sem, own_sem, load_sem), held, (lhs_t,), away, home, scratch = split(refs, num, 1, 3, 1, 5, num, 1, 2, 2)
    lhs, rhs, act, down, hidden, spread_m = held
    bits = own_bits()
    load = pltpu.make_async_copy(rows_ref, stage, own_sem.at[0])
    load.start()
    loads = [pltpu.make_async_copy(ins[i], held[i], load_sem.at[i]) for i in range(num)]
    for copy in loads:
        copy.start()
    tree = LastTree(bits, ATT_PIECES, dict(zip(LAST, (None, out_ref, small_ref))), dict(zip(LAST, results)), scratch)
    tree.multiply(lhs_t, rhs, away, home)
    tree.load()
    greet(bits)
    ring = Doubling(bits, ROW_PIECES, (rows_ref,), (all_ref,), rows_of, send_sem, recv_sem)
    ring.open()
    for copy in loads:
        copy.wait()

    def turn(i, carry):
        at = pl.ds(pl.multiple_of(i * LANES, LANES), LANES)
        lhs_t[at, :] = lhs[:, at].T
        return carry

    loop(DP // LANES, turn)
    tree.open()
    load.wait()
    store = pltpu.make_async_copy(stage, all_ref.at[device_at(bits, '')], own_sem.at[1])
    store.start()
    blocks = SEQ // HALF

    def project(i, carry):
        tokens = pl.ds(pl.multiple_of(i * HALF, HALF), HALF)
        total = (hidden[tokens, :].astype(jnp.float32) + dot_nn(act[tokens, :], down[...])).astype(jnp.bfloat16)
        part = pl.ds(pl.multiple_of((i % blocks) * HALF, HALF), HALF)
        y_ref[i // blocks, :, part] = dot_nt(spread_m[...], total).astype(jnp.bfloat16)
        return carry

    for n in range(len(FIRST_ORDER)):
        tree.first(n, tree.fill)
    ring.forward(1)
    ring.forward(2)
    ring.forward(3)
    tree.second()
    loop(TOKS // HALF, project)
    ring.forward(4)
    ring.forward(5)
    ring.forward(6)
    tree.third()
    ring.forward(7)
    tree.last(tree.put)
    tree.close()
    ring.close()
    store.wait()


def back(*operands):
    held = operands[3:]
    scratch = [pltpu.VMEM((TOKS, UNROLL, LANES), jnp.float32)] + sems(len(ROW_PIECES)) + [pltpu.SemaphoreType.DMA((2,)), pltpu.SemaphoreType.DMA((len(held),))]
    scratch += [pltpu.VMEM(array.shape, array.dtype) for array in held]
    scratch += [pltpu.VMEM((DP, TOKS), jnp.bfloat16)]
    scratch += [pltpu.VMEM((UNROLL, SUBP, piece[2]), jnp.float32) for piece in QKV_PIECES[:2]] * 2
    return pl.pallas_call(
        back_body,
        out_shape=(jax.ShapeDtypeStruct((SHARDS, TOKS, UNROLL, LANES), jnp.float32), *(grad_shape(a) for a in LAST), jax.ShapeDtypeStruct((TOKS // SEQ, D, SEQ), jnp.bfloat16)),
        in_specs=[ANY_SPEC] * len(operands),
        out_specs=(ANY_SPEC,) + (VMEM_SPEC,) * 4,
        scratch_shapes=scratch + tree_scratch(ATT_PIECES),
        compiler_params=comm(3, 60),
        cost_estimate=cost(80),
        name='back',
    )(*operands)


def spread_matrix():
    src = lax.broadcasted_iota(jnp.int32, (D, DP), 0)
    dst = lax.broadcasted_iota(jnp.int32, (D, DP), 1)
    return ((src // SUB) * SUBP + src % SUB == dst).astype(jnp.bfloat16)


def heads_matrix():
    src = lax.broadcasted_iota(jnp.int32, (KV_HEADS * GROUP_OUT, DP), 0)
    dst = lax.broadcasted_iota(jnp.int32, (KV_HEADS * GROUP_OUT, DP), 1)
    lane = src % GROUP_OUT
    feature = (src // GROUP_OUT) * GROUP * HEAD + lane
    return ((lane < GROUP * HEAD) & ((feature // SUB) * SUBP + feature % SUB == dst)).astype(jnp.bfloat16)


def matmul(spec, lhs, rhs):
    return jnp.einsum(spec, lhs, rhs, preferred_element_type=jnp.float32)


def spread(values, matrix):
    return matmul('...d,de->...e', values, matrix).astype(jnp.bfloat16)


def gather_back(values, matrix):
    return matmul('...e,de->...d', values, matrix).astype(jnp.bfloat16)


def unspread_columns(values):
    rows = values.shape[0]
    return values.reshape(rows, SHARDS, SUBP)[:, :, :SUB].reshape(rows, D)


def merge_groups(w_query, w_key, w_value, gains):
    parts = []
    for g in range(KV_HEADS):
        at = slice(g * HEAD, (g + 1) * HEAD)
        spare = jnp.pad(gains if g == 0 else gains[:, :0], ((0, 0), (0, HEAD - (2 if g == 0 else 0))))
        parts += [w_query[:, g * GROUP * HEAD:(g + 1) * GROUP * HEAD], w_key[:, at], w_value[:, at], spare]
    return jnp.concatenate(parts, axis=1)


def split_groups(merged):
    grouped = merged.reshape(merged.shape[0], KV_HEADS, GROUP_IN)
    edges = (0, GROUP * HEAD, (GROUP + 1) * HEAD, (GROUP + 2) * HEAD)
    return tuple(grouped[:, :, lo:hi].reshape(merged.shape[0], -1) for lo, hi in zip(edges, edges[1:]))


def sort_by_id(tok):
    row = lax.broadcasted_iota(jnp.int32, (TOKS, TOKS), 0)
    col = lax.broadcasted_iota(jnp.int32, (TOKS, TOKS), 1)
    ahead = (tok[None, :] < tok[:, None]) | ((tok[None, :] == tok[:, None]) & (col < row))
    place = jnp.sum(ahead.astype(jnp.int32), axis=1)
    edge = lax.broadcasted_iota(jnp.int32, (SHARDS, 1), 0) * ROWS_TABLE
    below = tok[None, :] < edge
    first = jnp.sum(below.astype(jnp.int32), axis=1)
    count = jnp.sum(((tok[None, :] < edge + ROWS_TABLE) & ~below).astype(jnp.int32), axis=1)
    local = tok % ROWS_TABLE
    halves = jnp.stack([local // HEAD, local % HEAD], axis=-1).astype(jnp.bfloat16)
    halves = matmul('st,tk->sk', (row == place[None, :]).astype(jnp.bfloat16), halves).astype(jnp.int32)
    return place, halves[:, 0] * HEAD + halves[:, 1], count, first


def order_body(place_ref, in_ref, out_ref):
    def step(i, carry):
        for k in range(UNROLL):
            t = i * UNROLL + k
            out_ref[place_ref[t]] = in_ref[t]
        return carry

    loop(TOKS // UNROLL, step)


def order_rows(place, rows):
    whole = pl.BlockSpec((TOKS, UNROLL, LANES), lambda i, *_: (0, 0, 0))
    return pl.pallas_call(
        order_body,
        grid_spec=pltpu.PrefetchScalarGridSpec(num_scalar_prefetch=1, grid=(1,), in_specs=[whole], out_specs=whole),
        out_shape=jax.ShapeDtypeStruct((TOKS, UNROLL, LANES), jnp.float32),
        compiler_params=pltpu.CompilerParams(vmem_limit_bytes=40 * MIB),
        name='order_rows',
    )(place, rows)


def add_body(ids_ref, first_ref, count_ref, in_ref, out_ref, acc):
    j = pl.program_id(0)
    first = first_ref[j]
    count = count_ref[j]

    @pl.when(j == 0)
    def _():
        def clear(i, carry):
            acc[pl.ds(i * UNROLL, UNROLL)] = jnp.zeros((UNROLL, UNROLL, LANES), jnp.float32)
            return carry

        loop(ROWS_TABLE // UNROLL, clear)

    def add(start, num):
        ids = [ids_ref[j * TOKS + start + k] for k in range(num)]
        olds = [acc[r] for r in ids]
        total = None
        totals = []
        for k in range(num):
            base = olds[k] if k == 0 else jnp.where(ids[k] == ids[k - 1], total, olds[k])
            total = base + in_ref[start + k]
            totals.append(total)
        for r, total in zip(ids, totals):
            acc[r] = total

    def step(i, carry):
        add(first + i * UNROLL, UNROLL)
        return carry

    def tail(i, carry):
        add(first + i, 1)
        return carry

    groups = count // UNROLL
    loop(groups, step)
    lax.fori_loop(groups * UNROLL, count, tail, 0)

    @pl.when(j == SHARDS - 1)
    def _():
        def flush(i, carry):
            at = pl.ds(pl.multiple_of(i * LANES, LANES), LANES)
            for k in range(UNROLL):
                block = acc[at, k, :].T
                for half in range(2):
                    out_ref[pl.ds((2 * k + half) * SUB, SUB), at] = block[half * SUBP:][:SUB]
            return carry

        loop(ROWS_TABLE // LANES, flush)


def add_rows(ids, first, count, rows):
    return pl.pallas_call(
        add_body,
        grid_spec=pltpu.PrefetchScalarGridSpec(
            num_scalar_prefetch=3, grid=(SHARDS,),
            in_specs=[pl.BlockSpec((TOKS, UNROLL, LANES), lambda j, *_: (j, 0, 0))],
            out_specs=pl.BlockSpec((D, ROWS_TABLE), lambda j, *_: (0, 0)),
            scratch_shapes=[pltpu.VMEM((ROWS_TABLE, UNROLL, LANES), jnp.float32)]),
        out_shape=jax.ShapeDtypeStruct((D, ROWS_TABLE), jnp.float32),
        compiler_params=pltpu.CompilerParams(vmem_limit_bytes=60 * MIB),
        name='add_rows',
    )(ids, first, count, rows)


def rope_tables(positions):
    half_dim = HEAD // 2
    inv_freq = jnp.exp(jnp.arange(half_dim, dtype=jnp.float32) * (-2.0 * math.log(ROPE_THETA) / HEAD))
    angles = positions.astype(jnp.float32)[:, :, None] * inv_freq
    cos_t, sin_t = jnp.cos(angles), jnp.sin(angles)
    return jnp.concatenate([cos_t, cos_t], axis=-1), jnp.concatenate([-sin_t, sin_t], axis=-1)


def swap_halves(values):
    half_dim = HEAD // 2
    return jnp.concatenate([values[:, half_dim:], values[:, :half_dim]], axis=-1)


def norm_fwd(values, width=HEAD):
    values_f = values.astype(jnp.float32)
    inv_rms = lax.rsqrt(jnp.sum(values_f * values_f, axis=-1, keepdims=True) * (1.0 / width) + NORM_EPS)
    return values_f * inv_rms, inv_rms


def norm_bwd(grad_out, normed, inv_rms, norm_gain, width=HEAD):
    grad_normed = grad_out * norm_gain.astype(jnp.float32)
    mean_term = jnp.sum(grad_normed * normed, axis=-1, keepdims=True) * (1.0 / width)
    return inv_rms * (grad_normed - normed * mean_term)


def rope_fwd(normed, gain, cos_w, sin_w):
    scaled = normed * gain
    return (scaled * cos_w + swap_halves(scaled) * sin_w).astype(jnp.bfloat16)


def dot_nt(lhs, rhs):
    return lax.dot_general(lhs, rhs, (((1,), (1,)), ((), ())), preferred_element_type=jnp.float32)


def dot_nn(lhs, rhs):
    return lax.dot_general(lhs, rhs, (((1,), (0,)), ((), ())), preferred_element_type=jnp.float32)


def dot_tn(lhs, rhs):
    return lax.dot_general(lhs, rhs, (((0,), (0,)), ((), ())), preferred_element_type=jnp.float32)


def mask_last(scores, axis):
    split = scores.shape[axis] - HALF
    key = lax.broadcasted_iota(jnp.int32, (HALF, HALF), axis)
    query = lax.broadcasted_iota(jnp.int32, (HALF, HALF), 1 - axis)
    last = jnp.where(key <= query, lax.slice_in_dim(scores, split, split + HALF, axis=axis), -1e30)
    if split == 0:
        return last
    return jnp.concatenate([lax.slice_in_dim(scores, 0, split, axis=axis), last], axis=axis)


def softmax_of(scores, axis):
    scores = mask_last(scores, axis)
    weights = jnp.exp(scores - jnp.max(scores, axis=axis, keepdims=True))
    return weights * (1.0 / jnp.sum(weights, axis=axis, keepdims=True))


def attn_fwd_unit(b, g, qkv_ref, cos_ref, sin_ref, gq_ref, gk_ref, o_ref, block):
    cos_w, sin_w = cos_ref[b], sin_ref[b]
    lanes_out = pl.ds(pl.multiple_of(g * GROUP_OUT, LANES), GROUP_OUT)
    all_heads = qkv_ref[b, :, pl.ds(pl.multiple_of(g * GROUP_IN, LANES), GROUP_IN)]
    k_rot = rope_fwd(norm_fwd(all_heads[:, K_LANES])[0], gk_ref[...], cos_w, sin_w)
    v_raw = all_heads[:, V_LANES]
    for r in range(GROUP):
        q_rot = rope_fwd(norm_fwd(all_heads[:, Q_LANES[r]])[0], gq_ref[...], cos_w, sin_w) * SCALE
        for lo in range(0, SEQ, HALF):
            hi = lo + HALF
            probs = softmax_of(dot_nt(k_rot[:hi], q_rot[lo:hi]), 0)
            block[lo:hi, Q_LANES[r]] = dot_tn(probs.astype(jnp.bfloat16), v_raw[:hi]).astype(jnp.bfloat16)
    block[:, K_LANES] = jnp.zeros((SEQ, HEAD), jnp.bfloat16)
    o_ref[b, :, lanes_out] = block[...]


def attn_fwd_body(*refs):
    num = len(MIDDLE)
    ins, shard_refs, (o_ref,), full_refs, (block,), stage, marks = split(refs, 5, num, 1, num, 1, num)
    w_send, w_recv, load_sem, store_sem = marks
    bits = own_bits()
    shards = OwnShards(bits, shard_refs, full_refs, stage, load_sem, store_sem)
    shards.load()
    greet(bits)
    ring = Doubling(bits, UP_PIECES, shard_refs, full_refs, columns_of, w_send, w_recv)
    ring.open()
    shards.store()

    def unit(i, carry):
        attn_fwd_unit(i // KV_HEADS, i % KV_HEADS, *ins, o_ref, block)
        for code, turn in enumerate(FORWARD_AT, 1):
            @pl.when(i == turn)
            def _(code=code):
                ring.forward(code)

        return carry

    loop(ins[0].shape[0] * KV_HEADS, unit)
    ring.forward(UNROLL - 1)
    ring.close()
    shards.close()


def attn_bwd_unit(b, g, qkv_ref, cos_ref, sin_ref, gq_ref, gk_ref, do_ref, d_ref, dgq_ref, dgk_ref, block, dq_acc, dk_acc, dv_acc):
    cos_w, sin_w = cos_ref[b], sin_ref[b]
    gain_q, gain_k = gq_ref[...], gk_ref[...]
    lanes_in = pl.ds(pl.multiple_of(g * GROUP_IN, LANES), GROUP_IN)
    lanes_out = pl.ds(pl.multiple_of(g * GROUP_OUT, LANES), GROUP_OUT)
    block[...] = qkv_ref[b, :, lanes_in]
    k_normed, k_inv = norm_fwd(block[:, K_LANES])
    k_rot = rope_fwd(k_normed, gain_k, cos_w, sin_w)
    k_scaled = k_rot * SCALE
    v_raw = block[:, V_LANES]
    all_grads = do_ref[b, :, lanes_out]
    dk_acc[...] = jnp.zeros_like(dk_acc)
    dv_acc[...] = jnp.zeros_like(dv_acc)
    gain_total = jnp.zeros((1, HEAD), jnp.float32)
    for r in range(GROUP):
        q_normed, q_inv = norm_fwd(block[:, Q_LANES[r]])
        q_rot = rope_fwd(q_normed, gain_q, cos_w, sin_w) * SCALE
        head_grad = all_grads[:, Q_LANES[r]]
        for lo in range(0, SEQ, HALF):
            hi = lo + HALF
            out_grad = head_grad[lo:hi]
            q_part = q_rot[lo:hi]
            probs = softmax_of(dot_nt(k_rot[:hi], q_part), 0)
            grad_probs = dot_nt(v_raw[:hi], out_grad)
            dv_acc[:hi] += dot_nn(probs.astype(jnp.bfloat16), out_grad)
            delta = jnp.sum(grad_probs * probs, axis=0, keepdims=True)
            grad_scores = (probs * (grad_probs - delta)).astype(jnp.bfloat16)
            dk_acc[:hi] += dot_nn(grad_scores, q_part)
            dq_acc[lo:hi] = dot_tn(grad_scores, k_scaled[:hi])
        grad_q = dq_acc[...]
        grad_q = grad_q * cos_w - swap_halves(grad_q) * sin_w
        gain_total = gain_total + jnp.sum(grad_q * q_normed, axis=0, keepdims=True)
        block[:, Q_LANES[r]] = norm_bwd(grad_q, q_normed, q_inv, gain_q).astype(jnp.bfloat16)
    grad_k = dk_acc[...]
    grad_k = grad_k * cos_w - swap_halves(grad_k) * sin_w
    dgq_ref[...] += gain_total
    dgk_ref[...] += jnp.sum(grad_k * k_normed, axis=0, keepdims=True)
    block[:, K_LANES] = norm_bwd(grad_k, k_normed, k_inv, gain_k).astype(jnp.bfloat16)
    block[:, V_LANES.start:] = jnp.concatenate([dv_acc[...], jnp.zeros((SEQ, HEAD), jnp.float32)], axis=-1).astype(jnp.bfloat16)
    d_ref[b, :, lanes_in] = block[...]


def attn_bwd_body(*refs):
    ins, (w_qkv,), grads, outs, (in_grad,), results, work, scratch = split(refs, 6, 1, 3, 3, 1, 3, 4)
    bits = own_bits()
    tree = GradTree(bits, MLP_PIECES, dict(zip(MLP, grads)), dict(zip(MLP, results)), scratch)
    tree.load()
    for ref in outs[1:]:
        ref[...] = jnp.zeros_like(ref)
    greet(bits)
    tree.open()
    tree.first(0, tree.fill)
    tree.first(1, tree.fill)

    def unit(i, carry):
        attn_bwd_unit(i // KV_HEADS, i % KV_HEADS, *ins, *outs, *work)
        for n in range(2, len(FIRST_ORDER)):
            @pl.when(i == n // 2 - 1)
            def _(n=n):
                tree.first(n, tree.fill)

        @pl.when(i == KV_HEADS)
        def _():
            tree.second()

        return carry

    loop(ins[0].shape[0] * KV_HEADS, unit)
    qkv_grad, blocks = outs[0], SEQ // HALF

    def input_grad(i, carry):
        rows = pl.ds(pl.multiple_of((i % blocks) * HALF, HALF), HALF)
        in_grad[i // blocks, rows, :] = dot_nt(qkv_grad[i // blocks, rows, :], w_qkv[...])
        return carry

    loop(blocks * qkv_grad.shape[0], input_grad)
    tree.third()
    tree.last(tree.put)
    tree.close()


def attn_fwd(qkv, tables, shards):
    stage, marks = shard_scratch(MIDDLE, len(UP_PIECES))
    return pl.pallas_call(
        attn_fwd_body,
        out_shape=(jax.ShapeDtypeStruct(qkv.shape[:2] + (KV_HEADS * GROUP_OUT,), jnp.bfloat16),) + tuple(gathered_shape(a) for a in MIDDLE),
        in_specs=[VMEM_SPEC] * (len(tables) + 1) + [ANY_SPEC] * len(shards),
        out_specs=(VMEM_SPEC,) + (ANY_SPEC,) * len(shards),
        scratch_shapes=[pltpu.VMEM((SEQ, GROUP_OUT), jnp.bfloat16)] + stage + marks,
        compiler_params=comm(4, 40),
        cost_estimate=cost(20),
        name='attn_fwd',
    )(qkv, *tables, *shards)


def attn_bwd(qkv, tables, w_qkv, grads):
    gain_shape = jax.ShapeDtypeStruct((1, HEAD), jnp.float32)
    return pl.pallas_call(
        attn_bwd_body,
        out_shape=(jax.ShapeDtypeStruct(qkv.shape, jnp.bfloat16), gain_shape, gain_shape, jax.ShapeDtypeStruct(qkv.shape[:2] + (DP,), jnp.float32), *(grad_shape(a) for a in MLP)),
        in_specs=[VMEM_SPEC] * (len(tables) + 2) + [ANY_SPEC] * len(grads),
        out_specs=(VMEM_SPEC,) * 7,
        scratch_shapes=[pltpu.VMEM((SEQ, GROUP_IN), jnp.bfloat16)] + [pltpu.VMEM((SEQ, HEAD), jnp.float32)] * 3 + tree_scratch(MLP_PIECES),
        compiler_params=comm(2, 63),
        cost_estimate=cost(60),
        name='attn_bwd',
    )(qkv, *tables, w_qkv, *grads)


def layer_fwd(x_emb, positions, weights, shards, dy_s):
    attn_norm, w_qkv, q_norm, k_norm, w_out, mlp_norm, w_down = weights
    cos_w, sin_w = rope_tables(positions)
    gain_q = q_norm.astype(jnp.float32)[None, :]
    gain_k = k_norm.astype(jnp.float32)[None, :]
    normed1, norm1_inv = norm_fwd(x_emb, D)
    attn_in = (normed1 * attn_norm.astype(jnp.float32)).astype(jnp.bfloat16)
    attn_args = (matmul('bsd,dn->bsn', attn_in, w_qkv).astype(jnp.bfloat16), cos_w, sin_w, gain_q, gain_k)
    heads, *full = attn_fwd(attn_args[0], attn_args[1:], shards)
    w_gate, w_up = (w.reshape(-1, w.shape[-1]) for w in full)
    attn_flat = spread(heads, heads_matrix())
    hidden = (x_emb.astype(jnp.float32) + matmul('bsn,nd->bsd', attn_flat, w_out)).astype(jnp.bfloat16)
    normed2, norm2_inv = norm_fwd(hidden, D)
    mlp_in = (normed2 * mlp_norm.astype(jnp.float32)).astype(jnp.bfloat16)
    gate_pre = matmul('bsd,df->bsf', mlp_in, w_gate)
    up_proj = matmul('bsd,df->bsf', mlp_in, w_up)
    gate_pre, up_proj, dy_s = lax.optimization_barrier((gate_pre, up_proj, dy_s))
    mlp_act = (jax.nn.silu(gate_pre) * up_proj).astype(jnp.bfloat16)
    return (mlp_act.reshape(TOKS, FF), w_down, hidden.reshape(TOKS, DP)), dy_s, (normed1, norm1_inv, attn_in, attn_args, attn_flat, normed2, norm2_inv, mlp_in, gate_pre, up_proj, mlp_act, w_gate, w_up)


def layer_bwd(dy_out, saved_acts, weights):
    attn_norm, w_qkv, q_norm, k_norm, w_out, mlp_norm, w_down = weights
    normed1, norm1_inv, attn_in, attn_args, attn_flat, normed2, norm2_inv, mlp_in, gate_pre, up_proj, mlp_act, w_gate, w_up = saved_acts
    grad_w_down = matmul('bsf,bsd->fd', mlp_act, dy_out)
    grad_act = matmul('bsd,fd->bsf', dy_out, w_down)
    gate_sig = jax.nn.sigmoid(gate_pre)
    grad_gate = (grad_act * up_proj * gate_sig * (1.0 + gate_pre * (1.0 - gate_sig))).astype(jnp.bfloat16)
    grad_up = (grad_act * gate_pre * gate_sig).astype(jnp.bfloat16)
    grad_w_gate = matmul('bsd,bsf->df', mlp_in, grad_gate)
    grad_w_up = matmul('bsd,bsf->df', mlp_in, grad_up)
    grad_mlp_in = matmul('bsf,df->bsd', grad_gate, w_gate) + matmul('bsf,df->bsd', grad_up, w_up)
    grad_mlp_norm = jnp.sum(grad_mlp_in * normed2, axis=(0, 1))
    grad_hidden = dy_out.astype(jnp.float32) + norm_bwd(grad_mlp_in, normed2, norm2_inv, mlp_norm, D)
    hidden_b = grad_hidden.astype(jnp.bfloat16)
    grad_w_out = matmul('bsn,bsd->nd', attn_flat, hidden_b)
    grad_heads = gather_back(matmul('bsd,nd->bsn', hidden_b, w_out).astype(jnp.bfloat16), heads_matrix())
    mlp_grads = [g.reshape(SHARDS, -1, g.shape[-1]) for g in (grad_w_gate, grad_w_up, grad_w_down)]
    grad_qkv, gains_q, gains_k, grad_attn_in, *mlp_shards = attn_bwd(attn_args[0], attn_args[1:] + (grad_heads,), w_qkv, mlp_grads)
    grad_attn_norm = jnp.sum(grad_attn_in * normed1, axis=(0, 1))
    grad_x_emb = grad_hidden + norm_bwd(grad_attn_in, normed1, norm1_inv, attn_norm, D)
    head_grads = [jnp.tile(gains[0], SHARDS) for gains in (gains_q, gains_k)]
    small = jnp.stack([grad_attn_norm, grad_mlp_norm] + head_grads, axis=-1)
    small = jnp.pad(small, ((0, 0), (0, COLS[5] - small.shape[-1])))
    parts = tuple(g.reshape(SHARDS, -1, g.shape[-1]) for g in (grad_w_out, small))
    return grad_x_emb, (*parts, attn_in.reshape(TOKS, DP), grad_qkv.reshape(TOKS, QKVP)), mlp_shards


def solution(mesh):
    row_spec = P(AXIS_NAME, None)
    vec_spec = P(AXIS_NAME)
    full_spec = P(None)
    batch_spec = P(AXIS_NAME, None, None)
    weight_specs = (vec_spec, row_spec, row_spec, row_spec, full_spec, full_spec, row_spec, vec_spec, row_spec, row_spec, row_spec)

    def device_step(tokens, positions, table_shard, attn_norm, w_query, w_key, w_value, q_norm, k_norm, w_out, mlp_norm, w_gate, w_up, w_down, dy_out):
        batch_len, seq_len = tokens.shape
        me = lax.axis_index(AXIS_NAME)
        tok = tokens.reshape(-1)
        place, ids, count, first = sort_by_id(tok)
        meta = lax.all_gather(jnp.concatenate([tok, ids, count, first, jnp.zeros((TOKS - 2 * SHARDS,), jnp.int32)]), AXIS_NAME)
        local = meta[:, :TOKS].reshape(-1) - me * ROWS_TABLE
        where = jnp.where((local >= 0) & (local < ROWS_TABLE), local, ROWS_TABLE)
        all_ids = meta[:, TOKS:2 * TOKS].reshape(-1)
        mine = lax.dynamic_index_in_dim(meta[:, 2 * TOKS:2 * TOKS + 2 * SHARDS].reshape(SHARDS, 2, SHARDS), me, 2, keepdims=False)
        sent, sent_first = mine[:, 0], mine[:, 1]
        spread_m = spread_matrix()
        table_rows = jnp.pad(table_shard, ((0, UNROLL), (0, DP - D))).reshape(ROWS_TABLE + UNROLL, UNROLL, LANES)
        pad_rows = ((0, SUBP - SUB), (0, 0))
        sh_qkv = merge_groups(w_query, w_key, w_value, jnp.stack([attn_norm, mlp_norm], axis=-1))
        *full, got = front(where, table_rows, (jnp.pad(sh_qkv, pad_rows), jnp.pad(spread(w_out, spread_m), pad_rows), spread(w_down, spread_m)))
        f_qkv, f_out, f_down = (w.reshape(-1, w.shape[-1]) for w in full)
        spare = GROUP_IN - HEAD
        weights = (f_qkv[:, spare], f_qkv, q_norm, k_norm, f_out, f_qkv[:, spare + 1], f_down)
        x_emb = spread(got.reshape(batch_len, seq_len, DP)[..., :D], spread_m)
        last, dy_s, saved_acts = layer_fwd(x_emb, positions, weights, [jnp.pad(w, pad_rows) for w in (w_gate, w_up)], spread(dy_out, spread_m))
        grad_x_emb, parts, (r_gate, r_up, r_down) = layer_bwd(dy_s, saved_acts, weights)
        grad_rows = grad_x_emb.reshape(TOKS, UNROLL, LANES)
        grad_rows = order_rows(place, grad_rows)
        all_rows, r_qkv, r_out, r_small, y_t = back(grad_rows, *parts, *last, spread_m)
        layer_out = y_t.transpose(0, 2, 1)
        d_table = add_rows(all_ids, sent_first, sent, all_rows.reshape(SHARDS * TOKS, UNROLL, LANES)).T
        g_query, g_key, g_value = split_groups(r_qkv[:SUB])
        g_attn, g_mlp, g_q, g_k = (r_small[:, i] for i in range(4))
        return (layer_out, d_table, g_attn[:SUB], g_query, g_key, g_value, g_q, g_k, unspread_columns(r_out[:SUB]), g_mlp[:SUB], r_gate[:SUB], r_up[:SUB], unspread_columns(r_down))

    return jax.shard_map(device_step, mesh=mesh, in_specs=(row_spec, row_spec, row_spec) + weight_specs + (batch_spec,), out_specs=(batch_spec, row_spec) + weight_specs, check_vma=False)
```
